128 devices in a mesh: groups: 4 (over x, y), traces: 32 (over z, core).
Axes of the slice: x: 2, y: 2, z: 16, core: 2. Of those that a mesh axis runs over, the one named last changes fastest.
The devices are a block of a 8x8x16 slice.
Arguments:
- raw_traces: float32 [32768, 8192], P(('groups', 'traces')), parts along dimension 0, may hold values from -6 to 6
- filter_index: int32 [32768], P(('groups', 'traces')), parts along dimension 0, may hold values from 0 to 255
- channel_order: int32 [1024], P('groups'), parts along dimension 0, may hold values from 0 to 255, each once
- wavelets: float32 [256, 256], P('traces'), may hold values from -0.375 to 0.375
- damping: float32 [256], P('traces'), may hold values from 0.02 to 0.5
Outputs:
- deconvolved: float32 [32768, 8192], P(('groups', 'traces')), parts along dimension 0
The draws below stay inside these ranges and needn't reach their ends.
There are 4 independent parts, one for each index of `groups`. The reference program is written for one: setup_inputs(seed, part) draws one part's arguments, and reference() takes and returns one part's arrays. A program takes and returns all parts, laid end to end along the dimension named above; an argument that names none is the same for every part. Nothing has to cross between parts.
Inputs may be any that keep to these rules, and one draw needn't show every extreme that they name: `channel_order`: each of 0 to 255 appears once.
All inputs are finite; a program needn't handle non-finite values.
Results may differ from the reference program's by a relative error of at most 0.00021.
Values sent between devices are 32-bit elements; how exact they have to be, the bound alone decides.
A program may use at most 192 MiB of HBM per device.

```python
import math
import jax
import jax.numpy as jnp
from jax import lax

L = 8192
FILTERS = 256
FLEN = 256
TR_DEV = 256
TRACES = 8192
N_TRACES = 32


def plant(drawn, own_key, smallest, largest):
    longest = drawn.shape.index(max(drawn.shape))
    spots = []
    for shift in (0, 1):
        where = [jax.random.randint(jax.random.fold_in(own_key, axis), (), 0, length) for axis, length in enumerate(drawn.shape)]
        where[longest] = (where[longest] + shift) % drawn.shape[longest]
        spots.append(tuple(where))
    return drawn.at[spots[0]].set(smallest).at[spots[1]].set(largest)


def block_scale(key, shape, pieces, least, largest):
    factor_of, own = 1.0, jax.random.fold_in(key, 6)
    for dim, blocks in pieces:
        steps = jnp.exp(jax.random.uniform(jax.random.fold_in(own, dim), (blocks,), jnp.float32, least / len(pieces), largest / len(pieces)))
        factor_of = factor_of * jnp.repeat(steps, shape[dim] // blocks).reshape([-1 if axis == dim else 1 for axis in range(len(shape))])
    return factor_of


def centred(key, dims, deviation, bound, pieces=(), kind=jnp.bfloat16):
    loudness = block_scale(key, dims, pieces, -0.22, 0.18) if pieces else 1.0
    array = jax.random.normal(key, dims, jnp.float32) * deviation * loudness
    return jnp.minimum(jnp.maximum(array, -bound), bound).astype(kind)


def setup_inputs(seed: int = 0, part: int = 0) -> dict:
    streams_of = jax.random.split(jax.random.key(seed), 6)
    part_keys = jax.random.split(jax.random.fold_in(streams_of[5], part), 6)
    return {
        "raw_traces": centred(part_keys[0], (TRACES, L), 1.0, 6.0, ((0, 32),), jnp.float32),
        "filter_index": plant(jax.random.randint(part_keys[1], (TRACES,), 0, FILTERS), jax.random.fold_in(part_keys[1], 1), 0, FILTERS - 1).astype(jnp.int32),
        "channel_order": jax.random.permutation(part_keys[2], TR_DEV).astype(jnp.int32),
        "wavelets": centred(streams_of[3], (FILTERS, FLEN), FLEN ** -0.5, 0.375, ((0, 32),), jnp.float32),
        "damping": jnp.clip(jnp.exp(math.log(0.5) - 3.218876 * jax.random.uniform(streams_of[4], (FILTERS,), jnp.float32) ** block_scale(streams_of[4], (FILTERS,), ((0, 32),), -0.2, 0.2)), 0.02, 0.5),
    }


def filter_gains(wavelets, damping):
    padded = jnp.pad(wavelets, ((0, 0), (0, L - FLEN)))
    spectrum = jnp.fft.fft(padded, axis=1)
    spec_re = jnp.real(spectrum)
    spec_im = jnp.imag(spectrum)
    power = spec_re * spec_re + spec_im * spec_im
    level = jnp.mean(power, axis=1, keepdims=True)
    denom = power + damping[:, None] * (level + 1e-6)
    return spec_re / denom, -spec_im / denom


def reference(raw_traces, filter_index, channel_order, wavelets, damping):
    gain_re, gain_im = filter_gains(wavelets, damping)
    blocks = raw_traces.reshape(N_TRACES, TR_DEV, L)
    picks = filter_index.reshape(N_TRACES, TR_DEV)

    def one_block(pair):
        rows, index = pair
        spectrum = jnp.fft.fft(rows, axis=1)
        spec_re = jnp.real(spectrum)
        spec_im = jnp.imag(spectrum)
        pick_re = jnp.take(gain_re, index, axis=0)
        pick_im = jnp.take(gain_im, index, axis=0)
        out_re = spec_re * pick_re - spec_im * pick_im
        out_im = spec_re * pick_im + spec_im * pick_re
        return jnp.real(jnp.fft.ifft(lax.complex(out_re, out_im), axis=1))

    results = lax.map(one_block, (blocks, picks)).reshape(TRACES, L)
    out_rows = jnp.arange(TRACES, dtype=jnp.int32)
    position = (out_rows // TR_DEV) * TR_DEV + jnp.take(channel_order, out_rows % TR_DEV).astype(jnp.int32)
    source = ((position % N_TRACES) * TR_DEV + position // N_TRACES).astype(jnp.int32)
    return jnp.take(results, source, axis=0)
```

```python
import functools
import math

import jax
import jax.numpy as jnp
import numpy as np
from jax import lax
from jax.experimental import pallas as pl
from jax.experimental.pallas import tpu as pltpu
from jax.sharding import PartitionSpec as P

MESH = pl.DeviceIdType.MESH
HIGHEST = lax.Precision.HIGHEST
HALF_ROOT = math.sqrt(0.5)

KEPT = [a + 8 * b for a in (1, 2, 3) for b in range(8)] + [8 * b for b in range(5)] + [4 + 8 * b for b in range(4)]
NK = len(KEPT)
CHUNK = 11
PITCH = 65
VMEM_LIMIT = 34 * 2**20


def tables():
    q = np.arange(128)
    turn = 2.0 * np.pi * (np.outer(q, q) % 128) / 128
    c, s = np.cos(turn), np.sin(turn)
    across = np.block([[c, -s], [s, c]]).astype(np.float32)
    twist = []
    for shift in (0, 128):
        angle = 2.0 * np.pi * (np.outer(KEPT, q + shift) % 8192) / 8192
        twist += [np.cos(angle), -np.sin(angle)]
    twist = np.stack(twist).astype(np.float32)
    return across, np.ascontiguousarray(np.broadcast_to(twist[:, :, None, :], (4, NK, 8, 128)))


def rotate(re, im, step):
    step %= 64
    if step == 0:
        return re, im
    c, s = math.cos(2 * math.pi * step / 64), math.sin(2 * math.pi * step / 64)
    return re * c + im * s, im * c - re * s


def four(x):
    (ar, ai), (br, bi), (cr, ci), (dr, di) = x
    sr, si, tr, ti = ar + cr, ai + ci, ar - cr, ai - ci
    ur, ui, vr, vi = br + dr, bi + di, br - dr, bi - di
    return [(sr + ur, si + ui), (tr + vi, ti - vr), (sr - ur, si - ui), (tr - vi, ti + vr)]


def eight(x):
    e, o = four(x[0::2]), four(x[1::2])
    r = HALF_ROOT
    w = [
        o[0],
        (r * (o[1][0] + o[1][1]), r * (o[1][1] - o[1][0])),
        (o[2][1], -o[2][0]),
        (r * (o[3][1] - o[3][0]), -r * (o[3][0] + o[3][1])),
    ]
    low = [(e[k][0] + w[k][0], e[k][1] + w[k][1]) for k in range(4)]
    high = [(e[k][0] - w[k][0], e[k][1] - w[k][1]) for k in range(4)]
    return low + high


def eight_real(x):
    s, t, u, v = x[0] + x[4], x[0] - x[4], x[2] + x[6], x[2] - x[6]
    s2, t2, u2, v2 = x[1] + x[5], x[1] - x[5], x[3] + x[7], x[3] - x[7]
    e0, o0 = s + u, s2 + u2
    wr, wi = HALF_ROOT * (t2 - v2), -HALF_ROOT * (t2 + v2)
    return [
        (e0 + o0, None),
        (t + wr, wi - v),
        (s - u, u2 - s2),
        (t - wr, v + wi),
        (e0 - o0, None),
    ]


def total(terms):
    terms = list(terms)
    while len(terms) > 1:
        terms = [terms[i] + terms[i + 1] if i + 1 < len(terms) else terms[i] for i in range(0, len(terms), 2)]
    return terms[0]


def rows_forward(x_ref, part, lhs):
    for b in range(8):
        v = eight_real([x_ref[:, pl.ds((8 * a + b) * 128, 128)] for a in range(8)])
        part[b, 0] = v[0][0]
        part[b, 7] = v[4][0]
        for k in (1, 2, 3):
            re, im = rotate(v[k][0], v[k][1], b * k)
            part[b, 2 * k - 1] = re
            part[b, 2 * k] = im
    for k in (1, 2, 3):
        out = eight([(part[b, 2 * k - 1], part[b, 2 * k]) for b in range(8)])
        for b in range(8):
            lhs[8 * (k - 1) + b, :, 0:128] = out[b][0]
            lhs[8 * (k - 1) + b, :, 128:256] = out[b][1]
    out = eight_real([part[b, 0] for b in range(8)])
    for b in range(5):
        lhs[24 + b, :, 0:128] = out[b][0]
        lhs[24 + b, :, 128:256] = jnp.zeros((8, 128), jnp.float32) if out[b][1] is None else out[b][1]
    real = [part[b, 7] for b in range(8)]
    for j in range(4):
        angles = [2 * math.pi * b * (2 * j + 1) / 16 for b in range(8)]
        lhs[29 + j, :, 0:128] = total(real[b] * math.cos(angles[b]) for b in range(8))
        lhs[29 + j, :, 128:256] = total(real[b] * -math.sin(angles[b]) for b in range(1, 8))


def rows_inverse(spec, part, out_ref):
    def at(i):
        return spec[i, :, 0:128], spec[i, :, 128:256]

    for k in (1, 2, 3):
        out = eight([at(8 * (k - 1) + b) for b in range(8)])
        for b in range(8):
            re, im = rotate(out[b][0], out[b][1], b * k)
            part[b, 2 * k - 1] = re
            part[b, 2 * k] = im
    zero = [at(24 + j) for j in range(5)]
    four_ = [at(29 + j) for j in range(4)]
    for b in range(8):
        terms = [zero[0][0], zero[4][0] if b % 2 == 0 else -zero[4][0]]
        for j in (1, 2, 3):
            terms.append(rotate(*zero[j], 8 * b * j)[0])
        part[b, 0] = total(terms)
        part[b, 7] = total(rotate(*four_[j], b * (4 + 8 * j))[0] for j in range(4))
    for b in range(8):
        e0, p1, m1, p2, m2, p3, m3, e4 = (part[b, i] for i in range(8))
        g0, g1 = e0 + e4, e0 - e4
        for a, base, turn in (
            (0, g0 + p2, p1 + p3),
            (2, g0 - p2, m1 - m3),
            (1, g1 + m2, HALF_ROOT * ((p1 + m1) + (m3 - p3))),
            (3, g1 - m2, HALF_ROOT * ((m1 - p1) + (p3 + m3))),
        ):
            out_ref[pl.ds(8 * a + b, 8, stride=PITCH), :] = base + turn
            out_ref[pl.ds(8 * (a + 4) + b, 8, stride=PITCH), :] = base - turn


def deconvolve(x_ref, out_ref, tap_ref, floor_ref, across, twist, part, lhs, spec):
    rows_forward(x_ref, part, lhs)
    h0, h1 = tap_ref[:, 0:128][None], tap_ref[:, 128:256][None]
    for at in range(0, NK, CHUNK):
        here = pl.ds(at, CHUNK)
        c, s = twist[0, here], twist[1, here]
        re, im = lhs[here, :, 0:128], lhs[here, :, 128:256]
        lhs[here, :, 0:128] = re * c - im * s
        lhs[here, :, 128:256] = re * s + im * c
        there = pl.ds(NK + at, CHUNK)
        lhs[there, :, 0:128] = h0 * c + h1 * twist[2, here]
        lhs[there, :, 128:256] = h0 * s + h1 * twist[3, here]
    both = jnp.dot(lhs[...].reshape(2 * NK * 8, 256), across[...], precision=HIGHEST, preferred_element_type=jnp.float32)
    spec[...] = both.reshape(2 * NK, 8, 256)
    floor = floor_ref[...][None]
    for at in range(0, NK, CHUNK):
        here, there = pl.ds(at, CHUNK), pl.ds(NK + at, CHUNK)
        xr, xi = spec[here, :, 0:128], spec[here, :, 128:256]
        hr, hi = spec[there, :, 0:128], spec[there, :, 128:256]
        scale = (2.0 / 8192) / ((hr * hr + hi * hi) + floor)
        lhs[here, :, 0:128] = (xr * hr + xi * hi) * scale
        lhs[here, :, 128:256] = (xr * hi - xi * hr) * scale
    back = jnp.dot(
        lhs[pl.ds(0, NK)].reshape(NK * 8, 256), across[...], precision=HIGHEST, preferred_element_type=jnp.float32
    )
    spec[pl.ds(0, NK)] = back.reshape(NK, 8, 256)
    for at in range(0, NK, CHUNK):
        here = pl.ds(at, CHUNK)
        c, s = twist[0, here], twist[1, here]
        re, im = spec[here, :, 0:128], spec[here, :, 128:256]
        spec[here, :, 0:128] = re * c - im * s
        spec[here, :, 128:256] = re * s + im * c
    for i in (24, 28):
        spec[i] = spec[i] * 0.5
    rows_inverse(spec, part, out_ref)


def exchange_kernel(
    n,
    x_ref, index_ref, damp_ref, wave_ref, across_ref, twist_ref,
    o_ref,
    raw, own, note, bank, taps, floors, across, twist, part, lhs, spec,
    send, recv, note_send, note_recv, wave_send, wave_recv, fours_send, fours_recv, pass_sem, own_sem, table_sem,
):
    me = lax.axis_index("traces")
    chips = n // 2
    z, core = me // 2, me % 2

    def place_of(z, core):
        return core * chips + (z % 4) * (chips // 4) + z // 4

    mine = place_of(z, core)

    def offset(k):
        later = (k + n - 4) // n
        dz = later * ((chips // 2 - k // 4) * (1 - 2 * (k % 2))) + (1 - later) * (chips // 2) * (k // 2)
        dc = later * ((k // 2) % 2) + (1 - later) * (k % 2)
        return dz, dc

    def target(k):
        dz, dc = offset(k)
        return ((z + dz + chips) % chips) * 2 + (core + dc) % 2

    def source(k):
        dz, dc = offset(k)
        return (z - dz + chips) % chips, (core + dc) % 2

    def eight_rows(i):
        return pl.ds(pl.multiple_of(i * 8, 8), 8)

    def raw_copy(k):
        t = target(k)
        return pltpu.make_async_remote_copy(
            src_ref=x_ref.at[eight_rows(t)], dst_ref=raw.at[k], send_sem=send.at[k], recv_sem=recv.at[k],
            device_id={"traces": t}, device_id_type=MESH,
        )

    def note_copy(k):
        t = target(k)
        return pltpu.make_async_remote_copy(
            src_ref=own.at[t], dst_ref=note.at[mine], send_sem=note_send.at[k], recv_sem=note_recv.at[k],
            device_id={"traces": t}, device_id_type=MESH,
        )

    def wave_copy(j):
        return pltpu.make_async_remote_copy(
            src_ref=wave_ref, dst_ref=bank.at[core, z % 4, z // 4], send_sem=wave_send.at[j], recv_sem=wave_recv.at[j],
            device_id={"traces": ((z + 4 * j) % chips) * 2 + core}, device_id_type=MESH,
        )

    def fours_copy(j):
        away = (0, 1, 2, chips - 1)[j]
        return pltpu.make_async_remote_copy(
            src_ref=bank.at[core, z % 4], dst_ref=bank.at[core, z % 4], send_sem=fours_send.at[j], recv_sem=fours_recv.at[j],
            device_id={"traces": ((z + away) % chips) * 2 + core}, device_id_type=MESH,
        )

    def pass_copy():
        return pltpu.make_async_remote_copy(
            src_ref=bank.at[core], dst_ref=bank.at[core], send_sem=pass_sem.at[0], recv_sem=pass_sem.at[1],
            device_id={"traces": z * 2 + 1 - core}, device_id_type=MESH,
        )

    barrier = pltpu.get_barrier_semaphore()

    def greet(k, _):
        pl.semaphore_signal(barrier, inc=1, device_id={"traces": target(k)}, device_id_type=MESH)
        return 0

    lax.fori_loop(1, n, greet, 0)
    own_copy = pltpu.make_async_copy(x_ref.at[eight_rows(me)], raw.at[0], own_sem)
    own_copy.start()
    across_copy = pltpu.make_async_copy(across_ref, across, table_sem.at[0])
    across_copy.start()
    twist_copy = pltpu.make_async_copy(twist_ref, twist, table_sem.at[1])
    twist_copy.start()
    bank[core, z % 4, z // 4] = wave_ref[...]
    lane = lax.broadcasted_iota(jnp.int32, (1, 128), 1)
    damp = jnp.zeros((1, 128), jnp.float32)
    for i in range(8):
        damp = jnp.where(lane == 8 + i, damp_ref[i], damp)

    def fill(e, _):
        row = damp
        for i in range(8):
            row = jnp.where(lane == i, index_ref[e * 8 + i].astype(jnp.float32), row)
        own[e] = row
        return 0

    lax.fori_loop(0, n, fill, 0)
    note[mine] = own[me]
    pl.semaphore_wait(barrier, n - 1)

    def start_note(k, _):
        note_copy(k).start()
        return 0

    def start_wave(j, _):
        wave_copy(j).start()
        return 0

    def start_raw(k, _):
        raw_copy(k).start()
        return 0

    def wait_wave(j, _):
        wave_copy(j).wait()
        return 0

    def wait_note(k, _):
        note_copy(k).wait()
        return 0

    lax.fori_loop(1, chips // 4, start_wave, 0)
    lax.fori_loop(1, n, start_note, 0)
    lax.fori_loop(1, 8, start_raw, 0)
    own_copy.wait()
    across_copy.wait()
    twist_copy.wait()
    lax.fori_loop(1, chips // 4, wait_wave, 0)
    for j in (1, 2, 3):
        fours_copy(j).start()
    lax.fori_loop(8, n, start_raw, 0)
    for j in (1, 2, 3):
        fours_copy(j).wait()
    pass_copy().start()
    lax.fori_loop(1, n, wait_note, 0)
    pass_copy().wait()

    notes = note[...]
    lanes = lax.broadcasted_iota(jnp.int32, (n, 8, 128), 2)
    place = lax.broadcasted_iota(jnp.int32, (n, 8, 128), 1)
    wanted = jnp.sum(jnp.where(lanes == place, notes, 0.0), axis=2, keepdims=True).reshape(8 * n, 1)
    damping = jnp.sum(jnp.where(lanes == place + 8, notes, 0.0), axis=2, keepdims=True).reshape(8 * n, 1)
    every = bank[...].reshape(8 * n, 256)
    level = jnp.sum(every * every, axis=1, keepdims=True)
    water = jnp.broadcast_to(damping * (level + 1e-6), (8 * n, 128))
    slot = lax.broadcasted_iota(jnp.int32, (8 * n, 8 * n), 1)
    chip = ((slot // 8) % (chips // 4)) * 4 + (slot // (2 * chips)) % 4
    ids = chip * 16 + (slot // (8 * chips)) * 8 + slot % 8
    pick = jnp.where(wanted == ids.astype(jnp.float32), 1.0, 0.0).astype(jnp.float32)
    taps[...] = jnp.dot(pick, every, precision=HIGHEST, preferred_element_type=jnp.float32).reshape(n, 8, 256)
    floors[...] = jnp.dot(pick, water, precision=HIGHEST, preferred_element_type=jnp.float32).reshape(n, 8, 128)

    def block(k, _):
        @pl.when(k > 0)
        def _():
            raw_copy(k).wait_recv()

        sz, sc = source(k)
        p = place_of(sz, sc)
        deconvolve(raw.at[k], o_ref.at[sz * 2 + sc], taps.at[p], floors.at[p], across, twist, part, lhs, spec)
        return 0

    lax.fori_loop(0, n, block, 0)

    def finish(k, _):
        raw_copy(k).wait_send()
        return 0

    lax.fori_loop(1, n, finish, 0)


def exchange(n, x, index, damp, wave, across, twist):
    rows, length = x.shape
    hbm = pl.BlockSpec(memory_space=pltpu.HBM)
    smem = pl.BlockSpec(memory_space=pltpu.SMEM)
    f32 = jnp.float32
    dma = pltpu.SemaphoreType.DMA
    return pl.pallas_call(
        functools.partial(exchange_kernel, n),
        out_shape=jax.ShapeDtypeStruct((n, 8 * PITCH, 128), f32),
        in_specs=[hbm, smem, smem, pl.BlockSpec(memory_space=pltpu.VMEM), hbm, hbm],
        out_specs=pl.BlockSpec(memory_space=pltpu.VMEM),
        scratch_shapes=[
            pltpu.VMEM((n, 8, length), f32),
            pltpu.VMEM((n, 1, 128), f32),
            pltpu.VMEM((n, 1, 128), f32),
            pltpu.VMEM((2, 4, n // 8, 8, 256), f32),
            pltpu.VMEM((n, 8, 256), f32),
            pltpu.VMEM((n, 8, 128), f32),
            pltpu.VMEM(across.shape, f32),
            pltpu.VMEM(twist.shape, f32),
            pltpu.VMEM((8, 8, 8, 128), f32),
            pltpu.VMEM((2 * NK, 8, 256), f32),
            pltpu.VMEM((2 * NK, 8, 256), f32),
            dma((n,)), dma((n,)), dma((n,)), dma((n,)), dma((n // 8,)), dma((n // 8,)), dma((4,)), dma((4,)), dma((2,)),
            dma, dma((2,)),
        ],
        compiler_params=pltpu.CompilerParams(collective_id=0, has_side_effects=True, vmem_limit_bytes=VMEM_LIMIT),
    )(*(pltpu.with_memory_space_constraint(a, pltpu.HBM) for a in (x, index, damp, wave, across, twist)))


def reorder_kernel(n, order_ref, x_ref, o_ref, held, lined, out_sem):
    rows = o_ref.shape[0]
    tiles = rows // 8

    def out_copy(t):
        here = pl.ds(pl.multiple_of(t * 8, 8), 8)
        return pltpu.make_async_copy(lined.at[here], o_ref.at[here], out_sem.at[t])

    def line_up(t, _):
        for i in range(8):
            p = order_ref[t * 8 + i]
            held[pl.ds(i * PITCH, 64), :] = x_ref[p % n, pl.ds((p // n) * PITCH, 64), :]
        here = pl.ds(pl.multiple_of(t * 8, 8), 8)
        for i in range(64):
            lined[here, pl.ds(i * 128, 128)] = held[pl.ds(i, 8, stride=PITCH), :]
        out_copy(t).start()
        return 0

    lax.fori_loop(0, tiles, line_up, 0)

    def finish(t, _):
        out_copy(t).wait()
        return 0

    lax.fori_loop(0, tiles, finish, 0)


def reorder(n, order, x):
    rows, length = order.shape[0], 8192
    return pl.pallas_call(
        functools.partial(reorder_kernel, n),
        out_shape=jax.ShapeDtypeStruct((rows, length), x.dtype),
        in_specs=[pl.BlockSpec(memory_space=pltpu.SMEM), pl.BlockSpec(memory_space=pltpu.VMEM)],
        out_specs=pl.BlockSpec(memory_space=pl.ANY),
        scratch_shapes=[
            pltpu.VMEM((8 * PITCH, 128), x.dtype),
            pltpu.VMEM((rows, length), x.dtype),
            pltpu.SemaphoreType.DMA((rows // 8,)),
        ],
        compiler_params=pltpu.CompilerParams(vmem_limit_bytes=VMEM_LIMIT),
    )(pltpu.with_memory_space_constraint(order, pltpu.HBM), x)


def solution(mesh):
    n = mesh.shape["traces"]
    across, twist = tables()

    def local(raw_traces, filter_index, channel_order, wavelets, damping):
        moved = exchange(n, raw_traces, filter_index, damping, wavelets, jnp.asarray(across), jnp.asarray(twist))
        return reorder(n, channel_order, moved)

    placed = (
        P(("groups", "traces"), None),
        P(("groups", "traces")),
        P("groups"),
        P("traces", None),
        P("traces"),
    )
    return jax.shard_map(
        local, mesh=mesh, in_specs=placed, out_specs=P(("groups", "traces"), None), check_vma=False
    )
```

```python
import functools
import math

import jax
import jax.numpy as jnp
import numpy as np
from jax import lax
from jax.experimental import pallas as pl
from jax.experimental.pallas import tpu as pltpu
from jax.sharding import PartitionSpec as P

MESH = pl.DeviceIdType.MESH
HIGHEST = lax.Precision.HIGHEST
HALF_ROOT = math.sqrt(0.5)

KEPT = [a + 8 * b for a in (1, 2, 3) for b in range(8)] + [8 * b for b in range(5)] + [4 + 8 * b for b in range(4)]
NK = len(KEPT)
CHUNK = 11
PITCH = 65
VMEM_LIMIT = 34 * 2**20
LATE = 8


def tables():
    q = np.arange(128)
    turn = 2.0 * np.pi * (np.outer(q, q) % 128) / 128
    c, s = np.cos(turn), np.sin(turn)
    across = np.block([[c, -s], [s, c]]).astype(np.float32)
    twist = []
    for shift in (0, 128):
        angle = 2.0 * np.pi * (np.outer(KEPT, q + shift) % 8192) / 8192
        twist += [np.cos(angle), -np.sin(angle)]
    twist = np.stack(twist).astype(np.float32)
    return across, np.ascontiguousarray(np.broadcast_to(twist[:, :, None, :], (4, NK, 8, 128)))


def rotate(re, im, step):
    step %= 64
    if step == 0:
        return re, im
    c, s = math.cos(2 * math.pi * step / 64), math.sin(2 * math.pi * step / 64)
    return re * c + im * s, im * c - re * s


def four(x):
    (ar, ai), (br, bi), (cr, ci), (dr, di) = x
    sr, si, tr, ti = ar + cr, ai + ci, ar - cr, ai - ci
    ur, ui, vr, vi = br + dr, bi + di, br - dr, bi - di
    return [(sr + ur, si + ui), (tr + vi, ti - vr), (sr - ur, si - ui), (tr - vi, ti + vr)]


def eight(x):
    e, o = four(x[0::2]), four(x[1::2])
    r = HALF_ROOT
    w = [
        o[0],
        (r * (o[1][0] + o[1][1]), r * (o[1][1] - o[1][0])),
        (o[2][1], -o[2][0]),
        (r * (o[3][1] - o[3][0]), -r * (o[3][0] + o[3][1])),
    ]
    low = [(e[k][0] + w[k][0], e[k][1] + w[k][1]) for k in range(4)]
    high = [(e[k][0] - w[k][0], e[k][1] - w[k][1]) for k in range(4)]
    return low + high


def eight_real(x):
    s, t, u, v = x[0] + x[4], x[0] - x[4], x[2] + x[6], x[2] - x[6]
    s2, t2, u2, v2 = x[1] + x[5], x[1] - x[5], x[3] + x[7], x[3] - x[7]
    e0, o0 = s + u, s2 + u2
    wr, wi = HALF_ROOT * (t2 - v2), -HALF_ROOT * (t2 + v2)
    return [
        (e0 + o0, None),
        (t + wr, wi - v),
        (s - u, u2 - s2),
        (t - wr, v + wi),
        (e0 - o0, None),
    ]


def total(terms):
    terms = list(terms)
    while len(terms) > 1:
        terms = [terms[i] + terms[i + 1] if i + 1 < len(terms) else terms[i] for i in range(0, len(terms), 2)]
    return terms[0]


def rows_forward(x_ref, part, lhs):
    for b in range(8):
        v = eight_real([x_ref[:, pl.ds((8 * a + b) * 128, 128)] for a in range(8)])
        part[b, 0] = v[0][0]
        part[b, 7] = v[4][0]
        for k in (1, 2, 3):
            re, im = rotate(v[k][0], v[k][1], b * k)
            part[b, 2 * k - 1] = re
            part[b, 2 * k] = im
    for k in (1, 2, 3):
        out = eight([(part[b, 2 * k - 1], part[b, 2 * k]) for b in range(8)])
        for b in range(8):
            lhs[8 * (k - 1) + b, :, 0:128] = out[b][0]
            lhs[8 * (k - 1) + b, :, 128:256] = out[b][1]
    out = eight_real([part[b, 0] for b in range(8)])
    for b in range(5):
        lhs[24 + b, :, 0:128] = out[b][0]
        lhs[24 + b, :, 128:256] = jnp.zeros((8, 128), jnp.float32) if out[b][1] is None else out[b][1]
    real = [part[b, 7] for b in range(8)]
    for j in range(4):
        angles = [2 * math.pi * b * (2 * j + 1) / 16 for b in range(8)]
        lhs[29 + j, :, 0:128] = total(real[b] * math.cos(angles[b]) for b in range(8))
        lhs[29 + j, :, 128:256] = total(real[b] * -math.sin(angles[b]) for b in range(1, 8))


def rows_inverse(spec, part, out_ref):
    def at(i):
        return spec[i, :, 0:128], spec[i, :, 128:256]

    for k in (1, 2, 3):
        out = eight([at(8 * (k - 1) + b) for b in range(8)])
        for b in range(8):
            re, im = rotate(out[b][0], out[b][1], b * k)
            part[b, 2 * k - 1] = re
            part[b, 2 * k] = im
    zero = [at(24 + j) for j in range(5)]
    four_ = [at(29 + j) for j in range(4)]
    for b in range(8):
        terms = [zero[0][0], zero[4][0] if b % 2 == 0 else -zero[4][0]]
        for j in (1, 2, 3):
            terms.append(rotate(*zero[j], 8 * b * j)[0])
        part[b, 0] = total(terms)
        part[b, 7] = total(rotate(*four_[j], b * (4 + 8 * j))[0] for j in range(4))
    for b in range(8):
        e0, p1, m1, p2, m2, p3, m3, e4 = (part[b, i] for i in range(8))
        g0, g1 = e0 + e4, e0 - e4
        for a, base, turn in (
            (0, g0 + p2, p1 + p3),
            (2, g0 - p2, m1 - m3),
            (1, g1 + m2, HALF_ROOT * ((p1 + m1) + (m3 - p3))),
            (3, g1 - m2, HALF_ROOT * ((m1 - p1) + (p3 + m3))),
        ):
            out_ref[pl.ds(8 * a + b, 8, stride=PITCH), :] = base + turn
            out_ref[pl.ds(8 * (a + 4) + b, 8, stride=PITCH), :] = base - turn


def deconvolve(x_ref, out_ref, tap_ref, floor_ref, across, twist, part, lhs, spec):
    rows_forward(x_ref, part, lhs)
    h0, h1 = tap_ref[:, 0:128][None], tap_ref[:, 128:256][None]
    for at in range(0, NK, CHUNK):
        here = pl.ds(at, CHUNK)
        c, s = twist[0, here], twist[1, here]
        re, im = lhs[here, :, 0:128], lhs[here, :, 128:256]
        lhs[here, :, 0:128] = re * c - im * s
        lhs[here, :, 128:256] = re * s + im * c
        there = pl.ds(NK + at, CHUNK)
        lhs[there, :, 0:128] = h0 * c + h1 * twist[2, here]
        lhs[there, :, 128:256] = h0 * s + h1 * twist[3, here]
    both = jnp.dot(lhs[...].reshape(2 * NK * 8, 256), across[...], precision=HIGHEST, preferred_element_type=jnp.float32)
    spec[...] = both.reshape(2 * NK, 8, 256)
    floor = floor_ref[...][None]
    for at in range(0, NK, CHUNK):
        here, there = pl.ds(at, CHUNK), pl.ds(NK + at, CHUNK)
        xr, xi = spec[here, :, 0:128], spec[here, :, 128:256]
        hr, hi = spec[there, :, 0:128], spec[there, :, 128:256]
        scale = (2.0 / 8192) / ((hr * hr + hi * hi) + floor)
        lhs[here, :, 0:128] = (xr * hr + xi * hi) * scale
        lhs[here, :, 128:256] = (xr * hi - xi * hr) * scale
    back = jnp.dot(
        lhs[pl.ds(0, NK)].reshape(NK * 8, 256), across[...], precision=HIGHEST, preferred_element_type=jnp.float32
    )
    spec[pl.ds(0, NK)] = back.reshape(NK, 8, 256)
    for at in range(0, NK, CHUNK):
        here = pl.ds(at, CHUNK)
        c, s = twist[0, here], twist[1, here]
        re, im = spec[here, :, 0:128], spec[here, :, 128:256]
        spec[here, :, 0:128] = re * c - im * s
        spec[here, :, 128:256] = re * s + im * c
    for i in (24, 28):
        spec[i] = spec[i] * 0.5
    rows_inverse(spec, part, out_ref)


def exchange_kernel(
    n,
    x_ref, index_ref, damp_ref, wave_ref, across_ref, twist_ref,
    o_ref,
    raw, own, note, bank, taps, floors, across, twist, part, lhs, spec,
    send, recv, note_send, note_recv, wave_send, wave_recv, fours_send, fours_recv, pass_sem, own_sem, table_sem,
):
    me = lax.axis_index("traces")
    chips = n // 2
    z, core = me // 2, me % 2

    def place_of(z, core):
        return core * chips + (z % 4) * (chips // 4) + z // 4

    mine = place_of(z, core)

    def offset(k):
        later = (k + n - 4) // n
        dz = later * ((chips // 2 - k // 4) * (1 - 2 * (k % 2))) + (1 - later) * (chips // 2) * (k // 2)
        dc = later * ((k // 2) % 2) + (1 - later) * (k % 2)
        return dz, dc

    def target(k):
        dz, dc = offset(k)
        return ((z + dz + chips) % chips) * 2 + (core + dc) % 2

    def source(k):
        dz, dc = offset(k)
        return (z - dz + chips) % chips, (core + dc) % 2

    def eight_rows(i):
        return pl.ds(pl.multiple_of(i * 8, 8), 8)

    def raw_copy(k):
        t = target(k)
        return pltpu.make_async_remote_copy(
            src_ref=x_ref.at[eight_rows(t)], dst_ref=raw.at[k], send_sem=send.at[k], recv_sem=recv.at[k],
            device_id={"traces": t}, device_id_type=MESH,
        )

    def late_copy(k):
        return pltpu.make_async_remote_copy(
            src_ref=o_ref.at[k + LATE], dst_ref=o_ref.at[me], send_sem=send.at[k], recv_sem=recv.at[k],
            device_id={"traces": target(k)}, device_id_type=MESH,
        )

    def late_input(k):
        return pltpu.make_async_copy(x_ref.at[eight_rows(target(k))], raw.at[k], own_sem.at[k - (n - LATE)])

    def note_copy(k):
        t = target(k)
        return pltpu.make_async_remote_copy(
            src_ref=own.at[t], dst_ref=note.at[mine], send_sem=note_send.at[k], recv_sem=note_recv.at[k],
            device_id={"traces": t}, device_id_type=MESH,
        )

    def wave_copy(j):
        return pltpu.make_async_remote_copy(
            src_ref=wave_ref, dst_ref=bank.at[core, z % 4, z // 4], send_sem=wave_send.at[j], recv_sem=wave_recv.at[j],
            device_id={"traces": ((z + 4 * j) % chips) * 2 + core}, device_id_type=MESH,
        )

    def fours_copy(j):
        away = (0, 1, 2, chips - 1)[j]
        return pltpu.make_async_remote_copy(
            src_ref=bank.at[core, z % 4], dst_ref=bank.at[core, z % 4], send_sem=fours_send.at[j], recv_sem=fours_recv.at[j],
            device_id={"traces": ((z + away) % chips) * 2 + core}, device_id_type=MESH,
        )

    def pass_copy():
        return pltpu.make_async_remote_copy(
            src_ref=bank.at[core], dst_ref=bank.at[core], send_sem=pass_sem.at[0], recv_sem=pass_sem.at[1],
            device_id={"traces": z * 2 + 1 - core}, device_id_type=MESH,
        )

    away = [(chips // 2, 0), (chips // 2, 1)]
    for d in range(chips // 2 - 1, 0, -1):
        away += [(d, 0), (-d, 0), (d, 1), (-d, 1)]
    away.append((0, 1))
    cores = (core, 1 - core)
    barrier = pltpu.get_barrier_semaphore()
    for dz, dc in away:
        there = lax.rem(z + (dz + chips), chips) * 2 + cores[dc]
        pl.semaphore_signal(barrier, inc=1, device_id={"traces": there}, device_id_type=MESH)
    pl.semaphore_wait(barrier, n - 1)

    def start_note(k, _):
        note_copy(k).start()
        return 0

    def start_raw(k, _):
        raw_copy(k).start()
        return 0

    def start_late(k, _):
        late_copy(k).start()
        return 0

    def start_input(k, _):
        late_input(k).start()
        return 0

    def wait_note(k, _):
        note_copy(k).wait()
        return 0

    def wait_input(k, _):
        late_input(k).wait()
        return 0

    for j in range(1, chips // 4):
        wave_copy(j).start()
    for k in (4, 5):
        raw_copy(k).start()
    own_copy = pltpu.make_async_copy(x_ref.at[eight_rows(me)], raw.at[0], own_sem.at[LATE])
    own_copy.start()
    across_copy = pltpu.make_async_copy(across_ref, across, table_sem.at[0])
    across_copy.start()
    twist_copy = pltpu.make_async_copy(twist_ref, twist, table_sem.at[1])
    twist_copy.start()
    lax.fori_loop(n - LATE, n, start_input, 0)
    bank[core, z % 4, z // 4] = wave_ref[...]
    lane = lax.broadcasted_iota(jnp.int32, (1, 128), 1)
    damp = jnp.zeros((1, 128), jnp.float32)
    for i in range(8):
        damp = jnp.where(lane == 8 + i, damp_ref[i], damp)

    def fill(e, _):
        row = damp
        for i in range(8):
            row = jnp.where(lane == i, index_ref[e * 8 + i].astype(jnp.float32), row)
        own[e] = row
        return 0

    lax.fori_loop(0, n, fill, 0)
    note[mine] = own[me]
    for j in range(1, chips // 4):
        wave_copy(j).wait()
    for j in (1, 2, 3):
        fours_copy(j).start()
    lax.fori_loop(1, n, start_note, 0)
    lax.fori_loop(1, 4, start_raw, 0)
    lax.fori_loop(6, n - LATE, start_raw, 0)
    own_copy.wait()
    across_copy.wait()
    twist_copy.wait()
    lax.fori_loop(n - LATE, n, wait_input, 0)
    for j in (1, 2, 3):
        fours_copy(j).wait()
    pass_copy().start()
    lax.fori_loop(1, n, wait_note, 0)
    pass_copy().wait()

    lanes = lax.broadcasted_iota(jnp.int32, (n, 8, 128), 2)
    place = lax.broadcasted_iota(jnp.int32, (n, 8, 128), 1)

    def spread(notes, at):
        return jnp.sum(jnp.where(lanes == place + at, notes, 0.0), axis=2, keepdims=True).reshape(8 * n, 1)

    damping = spread(note[...], 8)
    every = bank[...].reshape(8 * n, 256)
    level = jnp.sum(every * every, axis=1, keepdims=True)
    water = jnp.broadcast_to(damping * (level + 1e-6), (8 * n, 128))
    slot = lax.broadcasted_iota(jnp.int32, (8 * n, 8 * n), 1)
    chip = ((slot // 8) % (chips // 4)) * 4 + (slot // (2 * chips)) % 4
    ids = chip * 16 + (slot // (8 * chips)) * 8 + slot % 8
    for half, notes in enumerate((note, own)):
        pick = jnp.where(spread(notes[...], 0) == ids.astype(jnp.float32), 1.0, 0.0).astype(jnp.float32)
        here = pl.ds(half * n, n)
        taps[here] = jnp.dot(pick, every, precision=HIGHEST, preferred_element_type=jnp.float32).reshape(n, 8, 256)
        floors[here] = jnp.dot(pick, water, precision=HIGHEST, preferred_element_type=jnp.float32).reshape(n, 8, 128)

    def block(i, _):
        k = (i + n - LATE) % n
        raws = (i + n - LATE) // n
        sz, sc = source(k)

        @pl.when(i > LATE)
        def _():
            raw_copy(k).wait_recv()

        @pl.when(i == LATE + 1)
        def _():
            lax.fori_loop(n - LATE, n, start_late, 0)

        out = raws * (sz * 2 + sc) + (1 - raws) * (n + i)
        p = raws * place_of(sz, sc) + (1 - raws) * (n + target(k))
        deconvolve(raw.at[k], o_ref.at[out], taps.at[p], floors.at[p], across, twist, part, lhs, spec)
        return 0

    lax.fori_loop(0, n, block, 0)

    def finish_raw(k, _):
        raw_copy(k).wait_send()
        return 0

    def finish_late(k, _):
        late_copy(k).wait()
        return 0

    lax.fori_loop(1, n - LATE, finish_raw, 0)
    lax.fori_loop(n - LATE, n, finish_late, 0)


def exchange(n, x, index, damp, wave, across, twist):
    rows, length = x.shape
    hbm = pl.BlockSpec(memory_space=pltpu.HBM)
    smem = pl.BlockSpec(memory_space=pltpu.SMEM)
    f32 = jnp.float32
    dma = pltpu.SemaphoreType.DMA
    return pl.pallas_call(
        functools.partial(exchange_kernel, n),
        out_shape=jax.ShapeDtypeStruct((n + LATE, 8 * PITCH, 128), f32),
        in_specs=[hbm, smem, smem, pl.BlockSpec(memory_space=pltpu.VMEM), hbm, hbm],
        out_specs=pl.BlockSpec(memory_space=pltpu.VMEM),
        scratch_shapes=[
            pltpu.VMEM((n, 8, length), f32),
            pltpu.VMEM((n, 1, 128), f32),
            pltpu.VMEM((n, 1, 128), f32),
            pltpu.VMEM((2, 4, n // 8, 8, 256), f32),
            pltpu.VMEM((2 * n, 8, 256), f32),
            pltpu.VMEM((2 * n, 8, 128), f32),
            pltpu.VMEM(across.shape, f32),
            pltpu.VMEM(twist.shape, f32),
            pltpu.VMEM((8, 8, 8, 128), f32),
            pltpu.VMEM((2 * NK, 8, 256), f32),
            pltpu.VMEM((2 * NK, 8, 256), f32),
            dma((n,)), dma((n,)), dma((n,)), dma((n,)), dma((n // 8,)), dma((n // 8,)), dma((4,)), dma((4,)), dma((2,)),
            dma((LATE + 1,)), dma((2,)),
        ],
        compiler_params=pltpu.CompilerParams(collective_id=0, has_side_effects=True, vmem_limit_bytes=VMEM_LIMIT),
    )(*(pltpu.with_memory_space_constraint(a, pltpu.HBM) for a in (x, index, damp, wave, across, twist)))


def reorder_kernel(n, order_ref, x_ref, o_ref, *scratch):
    *helds, lined, out_sem = scratch
    rows = o_ref.shape[0]
    tiles = rows // 8

    def out_copy(t):
        here = pl.ds(pl.multiple_of(t * 8, 8), 8)
        return pltpu.make_async_copy(lined.at[here], o_ref.at[here], out_sem.at[t])

    def line_up(g, _):
        for u, held in enumerate(helds):
            t = g * len(helds) + u
            for i in range(8):
                p = order_ref[t * 8 + i]
                held[pl.ds(i * PITCH, 64), :] = x_ref[p % n, pl.ds((p // n) * PITCH, 64), :]
        for u, held in enumerate(helds):
            t = g * len(helds) + u
            here = pl.ds(pl.multiple_of(t * 8, 8), 8)
            for i in range(64):
                lined[here, pl.ds(i * 128, 128)] = held[pl.ds(i, 8, stride=PITCH), :]
            out_copy(t).start()
        return 0

    lax.fori_loop(0, tiles // len(helds), line_up, 0)

    def finish(t, _):
        out_copy(t).wait()
        return 0

    lax.fori_loop(0, tiles, finish, 0)


def reorder(n, order, x):
    rows, length = order.shape[0], 8192
    return pl.pallas_call(
        functools.partial(reorder_kernel, n),
        out_shape=jax.ShapeDtypeStruct((rows, length), x.dtype),
        in_specs=[pl.BlockSpec(memory_space=pltpu.SMEM), pl.BlockSpec(memory_space=pltpu.VMEM)],
        out_specs=pl.BlockSpec(memory_space=pl.ANY),
        scratch_shapes=[
            *[pltpu.VMEM((8 * PITCH, 128), x.dtype)] * 4,
            pltpu.VMEM((rows, length), x.dtype),
            pltpu.SemaphoreType.DMA((rows // 8,)),
        ],
        compiler_params=pltpu.CompilerParams(vmem_limit_bytes=VMEM_LIMIT),
    )(pltpu.with_memory_space_constraint(order, pltpu.HBM), x)


def solution(mesh):
    n = mesh.shape["traces"]
    across, twist = tables()

    def local(raw_traces, filter_index, channel_order, wavelets, damping):
        moved = exchange(n, raw_traces, filter_index, damping, wavelets, jnp.asarray(across), jnp.asarray(twist))
        return reorder(n, channel_order, moved)

    placed = (
        P(("groups", "traces"), None),
        P(("groups", "traces")),
        P("groups"),
        P("traces", None),
        P("traces"),
    )
    return jax.shard_map(
        local, mesh=mesh, in_specs=placed, out_specs=P(("groups", "traces"), None), check_vma=False
    )
```

```python
import functools
import math

import jax
import jax.numpy as jnp
import numpy as np
from jax import lax
from jax.experimental import pallas as pl
from jax.experimental.pallas import tpu as pltpu
from jax.sharding import PartitionSpec as P

MESH = pl.DeviceIdType.MESH
HIGHEST = lax.Precision.HIGHEST
HALF_ROOT = math.sqrt(0.5)

KEPT = [a + 8 * b for a in (1, 2, 3) for b in range(8)] + [8 * b for b in range(5)] + [4 + 8 * b for b in range(4)]
NK = len(KEPT)
CHUNK = 11
PITCH = 65
VMEM_LIMIT = 34 * 2**20
LATE = 8


def tables():
    q = np.arange(128)
    turn = 2.0 * np.pi * (np.outer(q, q) % 128) / 128
    c, s = np.cos(turn), np.sin(turn)
    across = np.block([[c, -s], [s, c]]).astype(np.float32)
    twist = []
    for shift in (0, 128):
        angle = 2.0 * np.pi * (np.outer(KEPT, q + shift) % 8192) / 8192
        twist += [np.cos(angle), -np.sin(angle)]
    twist = np.stack(twist).astype(np.float32)
    return across, np.ascontiguousarray(np.broadcast_to(twist[:, :, None, :], (4, NK, 8, 128)))


def rotate(re, im, step):
    step %= 64
    if step == 0:
        return re, im
    c, s = math.cos(2 * math.pi * step / 64), math.sin(2 * math.pi * step / 64)
    return re * c + im * s, im * c - re * s


def four(x):
    (ar, ai), (br, bi), (cr, ci), (dr, di) = x
    sr, si, tr, ti = ar + cr, ai + ci, ar - cr, ai - ci
    ur, ui, vr, vi = br + dr, bi + di, br - dr, bi - di
    return [(sr + ur, si + ui), (tr + vi, ti - vr), (sr - ur, si - ui), (tr - vi, ti + vr)]


def eight(x):
    e, o = four(x[0::2]), four(x[1::2])
    r = HALF_ROOT
    w = [
        o[0],
        (r * (o[1][0] + o[1][1]), r * (o[1][1] - o[1][0])),
        (o[2][1], -o[2][0]),
        (r * (o[3][1] - o[3][0]), -r * (o[3][0] + o[3][1])),
    ]
    low = [(e[k][0] + w[k][0], e[k][1] + w[k][1]) for k in range(4)]
    high = [(e[k][0] - w[k][0], e[k][1] - w[k][1]) for k in range(4)]
    return low + high


def eight_real(x):
    s, t, u, v = x[0] + x[4], x[0] - x[4], x[2] + x[6], x[2] - x[6]
    s2, t2, u2, v2 = x[1] + x[5], x[1] - x[5], x[3] + x[7], x[3] - x[7]
    e0, o0 = s + u, s2 + u2
    wr, wi = HALF_ROOT * (t2 - v2), -HALF_ROOT * (t2 + v2)
    return [
        (e0 + o0, None),
        (t + wr, wi - v),
        (s - u, u2 - s2),
        (t - wr, v + wi),
        (e0 - o0, None),
    ]


def total(terms):
    terms = list(terms)
    while len(terms) > 1:
        terms = [terms[i] + terms[i + 1] if i + 1 < len(terms) else terms[i] for i in range(0, len(terms), 2)]
    return terms[0]


def rows_forward(x_ref, part, lhs):
    for b in range(8):
        v = eight_real([x_ref[:, pl.ds((8 * a + b) * 128, 128)] for a in range(8)])
        part[b, 0] = v[0][0]
        part[b, 7] = v[4][0]
        for k in (1, 2, 3):
            re, im = rotate(v[k][0], v[k][1], b * k)
            part[b, 2 * k - 1] = re
            part[b, 2 * k] = im
    for k in (1, 2, 3):
        out = eight([(part[b, 2 * k - 1], part[b, 2 * k]) for b in range(8)])
        for b in range(8):
            lhs[8 * (k - 1) + b, :, 0:128] = out[b][0]
            lhs[8 * (k - 1) + b, :, 128:256] = out[b][1]
    out = eight_real([part[b, 0] for b in range(8)])
    for b in range(5):
        lhs[24 + b, :, 0:128] = out[b][0]
        lhs[24 + b, :, 128:256] = jnp.zeros((8, 128), jnp.float32) if out[b][1] is None else out[b][1]
    real = [part[b, 7] for b in range(8)]
    for j in range(4):
        angles = [2 * math.pi * b * (2 * j + 1) / 16 for b in range(8)]
        lhs[29 + j, :, 0:128] = total(real[b] * math.cos(angles[b]) for b in range(8))
        lhs[29 + j, :, 128:256] = total(real[b] * -math.sin(angles[b]) for b in range(1, 8))


def rows_inverse(spec, part, out_ref):
    def at(i):
        return spec[i, :, 0:128], spec[i, :, 128:256]

    for k in (1, 2, 3):
        out = eight([at(8 * (k - 1) + b) for b in range(8)])
        for b in range(8):
            re, im = rotate(out[b][0], out[b][1], b * k)
            part[b, 2 * k - 1] = re
            part[b, 2 * k] = im
    zero = [at(24 + j) for j in range(5)]
    four_ = [at(29 + j) for j in range(4)]
    for b in range(8):
        terms = [zero[0][0], zero[4][0] if b % 2 == 0 else -zero[4][0]]
        for j in (1, 2, 3):
            terms.append(rotate(*zero[j], 8 * b * j)[0])
        part[b, 0] = total(terms)
        part[b, 7] = total(rotate(*four_[j], b * (4 + 8 * j))[0] for j in range(4))
    for b in range(8):
        e0, p1, m1, p2, m2, p3, m3, e4 = (part[b, i] for i in range(8))
        g0, g1 = e0 + e4, e0 - e4
        for a, base, turn in (
            (0, g0 + p2, p1 + p3),
            (2, g0 - p2, m1 - m3),
            (1, g1 + m2, HALF_ROOT * ((p1 + m1) + (m3 - p3))),
            (3, g1 - m2, HALF_ROOT * ((m1 - p1) + (p3 + m3))),
        ):
            out_ref[pl.ds(8 * a + b, 8, stride=PITCH), :] = base + turn
            out_ref[pl.ds(8 * (a + 4) + b, 8, stride=PITCH), :] = base - turn


def deconvolve(x_ref, out_ref, tap_ref, floor_ref, across, twist, part, lhs, spec):
    rows_forward(x_ref, part, lhs)
    h0, h1 = tap_ref[:, 0:128][None], tap_ref[:, 128:256][None]
    for at in range(0, NK, CHUNK):
        here = pl.ds(at, CHUNK)
        c, s = twist[0, here], twist[1, here]
        re, im = lhs[here, :, 0:128], lhs[here, :, 128:256]
        lhs[here, :, 0:128] = re * c - im * s
        lhs[here, :, 128:256] = re * s + im * c
        there = pl.ds(NK + at, CHUNK)
        lhs[there, :, 0:128] = h0 * c + h1 * twist[2, here]
        lhs[there, :, 128:256] = h0 * s + h1 * twist[3, here]
    both = jnp.dot(lhs[...].reshape(2 * NK * 8, 256), across[...], precision=HIGHEST, preferred_element_type=jnp.float32)
    spec[...] = both.reshape(2 * NK, 8, 256)
    floor = floor_ref[...][None]
    for at in range(0, NK, CHUNK):
        here, there = pl.ds(at, CHUNK), pl.ds(NK + at, CHUNK)
        xr, xi = spec[here, :, 0:128], spec[here, :, 128:256]
        hr, hi = spec[there, :, 0:128], spec[there, :, 128:256]
        scale = (2.0 / 8192) / ((hr * hr + hi * hi) + floor)
        lhs[here, :, 0:128] = (xr * hr + xi * hi) * scale
        lhs[here, :, 128:256] = (xr * hi - xi * hr) * scale
    back = jnp.dot(
        lhs[pl.ds(0, NK)].reshape(NK * 8, 256), across[...], precision=HIGHEST, preferred_element_type=jnp.float32
    )
    spec[pl.ds(0, NK)] = back.reshape(NK, 8, 256)
    for at in range(0, NK, CHUNK):
        here = pl.ds(at, CHUNK)
        c, s = twist[0, here], twist[1, here]
        re, im = spec[here, :, 0:128], spec[here, :, 128:256]
        spec[here, :, 0:128] = re * c - im * s
        spec[here, :, 128:256] = re * s + im * c
    for i in (24, 28):
        spec[i] = spec[i] * 0.5
    rows_inverse(spec, part, out_ref)


def exchange_kernel(
    n,
    x_ref, index_ref, damp_ref, wave_ref, across_ref, twist_ref,
    o_ref,
    raw, own, note, bank, taps, floors, across, twist, part, lhs, spec,
    send, recv, note_send, note_recv, wave_send, wave_recv, fours_send, fours_recv, pass_sem, own_sem, table_sem, word,
):
    me = lax.axis_index("traces")
    chips = n // 2
    z, core = me // 2, me % 2

    def place_of(z, core):
        return core * chips + (z % 4) * (chips // 4) + z // 4

    mine = place_of(z, core)

    def offset(k):
        far = (k + n - 8) // n
        m = k // 2
        sign = 1 - 2 * (k % 2)
        near_dz = (m + 1) // 2 + (chips // 2 - 2) * (m // 3)
        one = ((m + 1) // 2) % 2
        near_dc = one * (m // 2) + (1 - one) * (k % 2)
        dz = sign * (far * (chips // 2 + 1 - k // 4) + (1 - far) * near_dz)
        dc = far * (m % 2) + (1 - far) * near_dc
        return dz, dc

    def target(k):
        dz, dc = offset(k)
        return ((z + dz + chips) % chips) * 2 + (core + dc) % 2

    def source(k):
        dz, dc = offset(k)
        return (z - dz + chips) % chips, (core + dc) % 2

    def eight_rows(i):
        return pl.ds(pl.multiple_of(i * 8, 8), 8)

    def raw_copy(k):
        t = target(k)
        return pltpu.make_async_remote_copy(
            src_ref=x_ref.at[eight_rows(t)], dst_ref=raw.at[k], send_sem=send.at[k], recv_sem=recv.at[k],
            device_id={"traces": t}, device_id_type=MESH,
        )

    def late_copy(k):
        return pltpu.make_async_remote_copy(
            src_ref=o_ref.at[k + LATE], dst_ref=o_ref.at[me], send_sem=send.at[k], recv_sem=recv.at[k],
            device_id={"traces": target(k)}, device_id_type=MESH,
        )

    def late_input(k):
        return pltpu.make_async_copy(x_ref.at[eight_rows(target(k))], raw.at[k], own_sem.at[k - (n - LATE)])

    def note_copy(k):
        t = target(k)
        return pltpu.make_async_remote_copy(
            src_ref=own.at[t], dst_ref=note.at[mine], send_sem=note_send.at[k], recv_sem=note_recv.at[k],
            device_id={"traces": t}, device_id_type=MESH,
        )

    def wave_copy(j):
        return pltpu.make_async_remote_copy(
            src_ref=wave_ref, dst_ref=bank.at[core, z % 4, z // 4], send_sem=wave_send.at[j], recv_sem=wave_recv.at[j],
            device_id={"traces": ((z + 4 * j) % chips) * 2 + core}, device_id_type=MESH,
        )

    def fours_copy(j):
        away = (0, 1, 2, chips - 1)[j]
        return pltpu.make_async_remote_copy(
            src_ref=bank.at[core, z % 4], dst_ref=bank.at[core, z % 4], send_sem=fours_send.at[j], recv_sem=fours_recv.at[j],
            device_id={"traces": ((z + away) % chips) * 2 + core}, device_id_type=MESH,
        )

    def pass_copy():
        return pltpu.make_async_remote_copy(
            src_ref=bank.at[core], dst_ref=bank.at[core], send_sem=pass_sem.at[0], recv_sem=pass_sem.at[1],
            device_id={"traces": z * 2 + 1 - core}, device_id_type=MESH,
        )

    right = lax.rem(z + 1, chips) * 2
    left = lax.rem(z + (chips - 1), chips) * 2
    barrier = pltpu.get_barrier_semaphore()
    for there in (right + core, left + core, right + 1 - core, left + 1 - core, z * 2 + 1 - core):
        pl.semaphore_signal(barrier, inc=1, device_id={"traces": there}, device_id_type=MESH)
    pl.semaphore_wait(barrier, 5)

    def tell(side):
        there = (right if side == 0 else left) + core
        pl.semaphore_signal(word.at[side], inc=1, device_id={"traces": there}, device_id_type=MESH)

    tell(0)
    tell(1)
    for k in (2, 3, 4, 5, 1):
        raw_copy(k).start()

    def hear(_, __):
        for side in (0, 1):
            pl.semaphore_wait(word.at[side], 1)
            tell(side)
        return 0

    lax.fori_loop(0, chips // 2 - 2, hear, 0)
    for side in (0, 1):
        pl.semaphore_wait(word.at[side], 1)

    def start_note(k, _):
        note_copy(k).start()
        return 0

    def start_raw(k, _):
        raw_copy(k).start()
        return 0

    def start_late(k, _):
        late_copy(k).start()
        return 0

    def start_input(k, _):
        late_input(k).start()
        return 0

    def wait_note(k, _):
        note_copy(k).wait()
        return 0

    def wait_input(k, _):
        late_input(k).wait()
        return 0

    for j in range(1, chips // 4):
        wave_copy(j).start()
    for k in (8, 9):
        raw_copy(k).start()
    own_copy = pltpu.make_async_copy(x_ref.at[eight_rows(me)], raw.at[0], own_sem.at[LATE])
    own_copy.start()
    across_copy = pltpu.make_async_copy(across_ref, across, table_sem.at[0])
    across_copy.start()
    twist_copy = pltpu.make_async_copy(twist_ref, twist, table_sem.at[1])
    twist_copy.start()
    lax.fori_loop(n - LATE, n, start_input, 0)
    bank[core, z % 4, z // 4] = wave_ref[...]
    lane = lax.broadcasted_iota(jnp.int32, (1, 128), 1)
    damp = jnp.zeros((1, 128), jnp.float32)
    for i in range(8):
        damp = jnp.where(lane == 8 + i, damp_ref[i], damp)

    def fill(e, _):
        row = damp
        for i in range(8):
            row = jnp.where(lane == i, index_ref[e * 8 + i].astype(jnp.float32), row)
        own[e] = row
        return 0

    lax.fori_loop(0, n, fill, 0)
    note[mine] = own[me]
    for j in range(1, chips // 4):
        wave_copy(j).wait()
    for j in (1, 2, 3):
        fours_copy(j).start()
    lax.fori_loop(1, n, start_note, 0)
    lax.fori_loop(6, 8, start_raw, 0)
    lax.fori_loop(10, n - LATE, start_raw, 0)
    own_copy.wait()
    across_copy.wait()
    twist_copy.wait()
    lax.fori_loop(n - LATE, n, wait_input, 0)
    for j in (1, 2, 3):
        fours_copy(j).wait()
    pass_copy().start()
    lax.fori_loop(1, n, wait_note, 0)
    pass_copy().wait()

    lanes = lax.broadcasted_iota(jnp.int32, (n, 8, 128), 2)
    place = lax.broadcasted_iota(jnp.int32, (n, 8, 128), 1)

    def spread(notes, at):
        return jnp.sum(jnp.where(lanes == place + at, notes, 0.0), axis=2, keepdims=True).reshape(8 * n, 1)

    damping = spread(note[...], 8)
    every = bank[...].reshape(8 * n, 256)
    level = jnp.sum(every * every, axis=1, keepdims=True)
    water = jnp.broadcast_to(damping * (level + 1e-6), (8 * n, 128))
    slot = lax.broadcasted_iota(jnp.int32, (8 * n, 8 * n), 1)
    chip = ((slot // 8) % (chips // 4)) * 4 + (slot // (2 * chips)) % 4
    ids = chip * 16 + (slot // (8 * chips)) * 8 + slot % 8
    for half, notes in enumerate((note, own)):
        pick = jnp.where(spread(notes[...], 0) == ids.astype(jnp.float32), 1.0, 0.0).astype(jnp.float32)
        here = pl.ds(half * n, n)
        taps[here] = jnp.dot(pick, every, precision=HIGHEST, preferred_element_type=jnp.float32).reshape(n, 8, 256)
        floors[here] = jnp.dot(pick, water, precision=HIGHEST, preferred_element_type=jnp.float32).reshape(n, 8, 128)

    def block(i, _):
        k = (i + n - LATE) % n
        raws = (i + n - LATE) // n
        sz, sc = source(k)

        @pl.when(i > LATE)
        def _():
            raw_copy(k).wait_recv()

        @pl.when(i == LATE + 1)
        def _():
            lax.fori_loop(n - LATE, n, start_late, 0)

        out = raws * (sz * 2 + sc) + (1 - raws) * (n + i)
        p = raws * place_of(sz, sc) + (1 - raws) * (n + target(k))
        deconvolve(raw.at[k], o_ref.at[out], taps.at[p], floors.at[p], across, twist, part, lhs, spec)
        return 0

    lax.fori_loop(0, n, block, 0)

    def finish_raw(k, _):
        raw_copy(k).wait_send()
        return 0

    def finish_late(k, _):
        late_copy(k).wait()
        return 0

    lax.fori_loop(1, n - LATE, finish_raw, 0)
    lax.fori_loop(n - LATE, n, finish_late, 0)


def exchange(n, x, index, damp, wave, across, twist):
    rows, length = x.shape
    hbm = pl.BlockSpec(memory_space=pltpu.HBM)
    smem = pl.BlockSpec(memory_space=pltpu.SMEM)
    f32 = jnp.float32
    dma = pltpu.SemaphoreType.DMA
    return pl.pallas_call(
        functools.partial(exchange_kernel, n),
        out_shape=jax.ShapeDtypeStruct((n + LATE, 8 * PITCH, 128), f32),
        in_specs=[hbm, smem, smem, pl.BlockSpec(memory_space=pltpu.VMEM), hbm, hbm],
        out_specs=pl.BlockSpec(memory_space=pltpu.VMEM),
        scratch_shapes=[
            pltpu.VMEM((n, 8, length), f32),
            pltpu.VMEM((n, 1, 128), f32),
            pltpu.VMEM((n, 1, 128), f32),
            pltpu.VMEM((2, 4, n // 8, 8, 256), f32),
            pltpu.VMEM((2 * n, 8, 256), f32),
            pltpu.VMEM((2 * n, 8, 128), f32),
            pltpu.VMEM(across.shape, f32),
            pltpu.VMEM(twist.shape, f32),
            pltpu.VMEM((8, 8, 8, 128), f32),
            pltpu.VMEM((2 * NK, 8, 256), f32),
            pltpu.VMEM((2 * NK, 8, 256), f32),
            dma((n,)), dma((n,)), dma((n,)), dma((n,)), dma((n // 8,)), dma((n // 8,)), dma((4,)), dma((4,)), dma((2,)),
            dma((LATE + 1,)), dma((2,)), pltpu.SemaphoreType.REGULAR((2,)),
        ],
        compiler_params=pltpu.CompilerParams(collective_id=0, has_side_effects=True, vmem_limit_bytes=VMEM_LIMIT),
    )(*(pltpu.with_memory_space_constraint(a, pltpu.HBM) for a in (x, index, damp, wave, across, twist)))


def reorder_kernel(n, order_ref, x_ref, o_ref, *scratch):
    *helds, lined, out_sem = scratch
    rows = o_ref.shape[0]
    tiles = rows // 8

    def out_copy(t):
        here = pl.ds(pl.multiple_of(t * 8, 8), 8)
        return pltpu.make_async_copy(lined.at[here], o_ref.at[here], out_sem.at[t])

    def line_up(g, _):
        for u, held in enumerate(helds):
            t = g * len(helds) + u
            for i in range(8):
                p = order_ref[t * 8 + i]
                held[pl.ds(i * PITCH, 64), :] = x_ref[p % n, pl.ds((p // n) * PITCH, 64), :]
        for u, held in enumerate(helds):
            t = g * len(helds) + u
            here = pl.ds(pl.multiple_of(t * 8, 8), 8)
            for i in range(64):
                lined[here, pl.ds(i * 128, 128)] = held[pl.ds(i, 8, stride=PITCH), :]
            out_copy(t).start()
        return 0

    lax.fori_loop(0, tiles // len(helds), line_up, 0)

    def finish(t, _):
        out_copy(t).wait()
        return 0

    lax.fori_loop(0, tiles, finish, 0)


def reorder(n, order, x):
    rows, length = order.shape[0], 8192
    return pl.pallas_call(
        functools.partial(reorder_kernel, n),
        out_shape=jax.ShapeDtypeStruct((rows, length), x.dtype),
        in_specs=[pl.BlockSpec(memory_space=pltpu.SMEM), pl.BlockSpec(memory_space=pltpu.VMEM)],
        out_specs=pl.BlockSpec(memory_space=pl.ANY),
        scratch_shapes=[
            *[pltpu.VMEM((8 * PITCH, 128), x.dtype)] * 4,
            pltpu.VMEM((rows, length), x.dtype),
            pltpu.SemaphoreType.DMA((rows // 8,)),
        ],
        compiler_params=pltpu.CompilerParams(vmem_limit_bytes=VMEM_LIMIT),
    )(pltpu.with_memory_space_constraint(order, pltpu.HBM), x)


def solution(mesh):
    n = mesh.shape["traces"]
    across, twist = tables()

    def local(raw_traces, filter_index, channel_order, wavelets, damping):
        moved = exchange(n, raw_traces, filter_index, damping, wavelets, jnp.asarray(across), jnp.asarray(twist))
        return reorder(n, channel_order, moved)

    placed = (
        P(("groups", "traces"), None),
        P(("groups", "traces")),
        P("groups"),
        P("traces", None),
        P("traces"),
    )
    return jax.shard_map(
        local, mesh=mesh, in_specs=placed, out_specs=P(("groups", "traces"), None), check_vma=False
    )
```

```python
import functools
import math

import jax
import jax.numpy as jnp
import numpy as np
from jax import lax
from jax.experimental import pallas as pl
from jax.experimental.pallas import tpu as pltpu
from jax.sharding import PartitionSpec as P

MESH = pl.DeviceIdType.MESH
HIGHEST = lax.Precision.HIGHEST
HALF_ROOT = math.sqrt(0.5)

KEPT = [a + 8 * b for a in (1, 2, 3) for b in range(8)] + [8 * b for b in range(5)] + [4 + 8 * b for b in range(4)]
NK = len(KEPT)
CHUNK = 11
PITCH = 65
VMEM_LIMIT = 34 * 2**20
LATE = 8


def tables():
    q = np.arange(128)
    turn = 2.0 * np.pi * (np.outer(q, q) % 128) / 128
    c, s = np.cos(turn), np.sin(turn)
    across = np.block([[c, -s], [s, c]]).astype(np.float32)
    twist = []
    for shift in (0, 128):
        angle = 2.0 * np.pi * (np.outer(KEPT, q + shift) % 8192) / 8192
        twist += [np.cos(angle), -np.sin(angle)]
    twist = np.stack(twist).astype(np.float32)
    return across, np.ascontiguousarray(np.broadcast_to(twist[:, :, None, :], (4, NK, 8, 128)))


def rotate(re, im, step):
    step %= 64
    if step == 0:
        return re, im
    c, s = math.cos(2 * math.pi * step / 64), math.sin(2 * math.pi * step / 64)
    return re * c + im * s, im * c - re * s


def four(x):
    (ar, ai), (br, bi), (cr, ci), (dr, di) = x
    sr, si, tr, ti = ar + cr, ai + ci, ar - cr, ai - ci
    ur, ui, vr, vi = br + dr, bi + di, br - dr, bi - di
    return [(sr + ur, si + ui), (tr + vi, ti - vr), (sr - ur, si - ui), (tr - vi, ti + vr)]


def eight(x):
    e, o = four(x[0::2]), four(x[1::2])
    r = HALF_ROOT
    w = [
        o[0],
        (r * (o[1][0] + o[1][1]), r * (o[1][1] - o[1][0])),
        (o[2][1], -o[2][0]),
        (r * (o[3][1] - o[3][0]), -r * (o[3][0] + o[3][1])),
    ]
    low = [(e[k][0] + w[k][0], e[k][1] + w[k][1]) for k in range(4)]
    high = [(e[k][0] - w[k][0], e[k][1] - w[k][1]) for k in range(4)]
    return low + high


def eight_real(x):
    s, t, u, v = x[0] + x[4], x[0] - x[4], x[2] + x[6], x[2] - x[6]
    s2, t2, u2, v2 = x[1] + x[5], x[1] - x[5], x[3] + x[7], x[3] - x[7]
    e0, o0 = s + u, s2 + u2
    wr, wi = HALF_ROOT * (t2 - v2), -HALF_ROOT * (t2 + v2)
    return [
        (e0 + o0, None),
        (t + wr, wi - v),
        (s - u, u2 - s2),
        (t - wr, v + wi),
        (e0 - o0, None),
    ]


def total(terms):
    terms = list(terms)
    while len(terms) > 1:
        terms = [terms[i] + terms[i + 1] if i + 1 < len(terms) else terms[i] for i in range(0, len(terms), 2)]
    return terms[0]


def rows_forward(x_ref, part, lhs):
    for b in range(8):
        v = eight_real([x_ref[:, pl.ds((8 * a + b) * 128, 128)] for a in range(8)])
        part[b, 0] = v[0][0]
        part[b, 7] = v[4][0]
        for k in (1, 2, 3):
            re, im = rotate(v[k][0], v[k][1], b * k)
            part[b, 2 * k - 1] = re
            part[b, 2 * k] = im
    for k in (1, 2, 3):
        out = eight([(part[b, 2 * k - 1], part[b, 2 * k]) for b in range(8)])
        for b in range(8):
            lhs[8 * (k - 1) + b, :, 0:128] = out[b][0]
            lhs[8 * (k - 1) + b, :, 128:256] = out[b][1]
    out = eight_real([part[b, 0] for b in range(8)])
    for b in range(5):
        lhs[24 + b, :, 0:128] = out[b][0]
        lhs[24 + b, :, 128:256] = jnp.zeros((8, 128), jnp.float32) if out[b][1] is None else out[b][1]
    real = [part[b, 7] for b in range(8)]
    for j in range(4):
        angles = [2 * math.pi * b * (2 * j + 1) / 16 for b in range(8)]
        lhs[29 + j, :, 0:128] = total(real[b] * math.cos(angles[b]) for b in range(8))
        lhs[29 + j, :, 128:256] = total(real[b] * -math.sin(angles[b]) for b in range(1, 8))


def rows_inverse(spec, part, out_ref):
    def at(i):
        return spec[i, :, 0:128], spec[i, :, 128:256]

    for k in (1, 2, 3):
        out = eight([at(8 * (k - 1) + b) for b in range(8)])
        for b in range(8):
            re, im = rotate(out[b][0], out[b][1], b * k)
            part[b, 2 * k - 1] = re
            part[b, 2 * k] = im
    zero = [at(24 + j) for j in range(5)]
    four_ = [at(29 + j) for j in range(4)]
    for b in range(8):
        terms = [zero[0][0], zero[4][0] if b % 2 == 0 else -zero[4][0]]
        for j in (1, 2, 3):
            terms.append(rotate(*zero[j], 8 * b * j)[0])
        part[b, 0] = total(terms)
        part[b, 7] = total(rotate(*four_[j], b * (4 + 8 * j))[0] for j in range(4))
    for b in range(8):
        e0, p1, m1, p2, m2, p3, m3, e4 = (part[b, i] for i in range(8))
        g0, g1 = e0 + e4, e0 - e4
        for a, base, turn in (
            (0, g0 + p2, p1 + p3),
            (2, g0 - p2, m1 - m3),
            (1, g1 + m2, HALF_ROOT * ((p1 + m1) + (m3 - p3))),
            (3, g1 - m2, HALF_ROOT * ((m1 - p1) + (p3 + m3))),
        ):
            out_ref[pl.ds(8 * a + b, 8, stride=PITCH), :] = base + turn
            out_ref[pl.ds(8 * (a + 4) + b, 8, stride=PITCH), :] = base - turn


def deconvolve(x_ref, out_ref, tap_ref, floor_ref, across, twist, part, lhs, spec):
    rows_forward(x_ref, part, lhs)
    h0, h1 = tap_ref[:, 0:128][None], tap_ref[:, 128:256][None]
    for at in range(0, NK, CHUNK):
        here = pl.ds(at, CHUNK)
        c, s = twist[0, here], twist[1, here]
        re, im = lhs[here, :, 0:128], lhs[here, :, 128:256]
        lhs[here, :, 0:128] = re * c - im * s
        lhs[here, :, 128:256] = re * s + im * c
        there = pl.ds(NK + at, CHUNK)
        lhs[there, :, 0:128] = h0 * c + h1 * twist[2, here]
        lhs[there, :, 128:256] = h0 * s + h1 * twist[3, here]
    both = jnp.dot(lhs[...].reshape(2 * NK * 8, 256), across[...], precision=HIGHEST, preferred_element_type=jnp.float32)
    spec[...] = both.reshape(2 * NK, 8, 256)
    floor = floor_ref[...][None]
    for at in range(0, NK, CHUNK):
        here, there = pl.ds(at, CHUNK), pl.ds(NK + at, CHUNK)
        xr, xi = spec[here, :, 0:128], spec[here, :, 128:256]
        hr, hi = spec[there, :, 0:128], spec[there, :, 128:256]
        scale = (2.0 / 8192) / ((hr * hr + hi * hi) + floor)
        lhs[here, :, 0:128] = (xr * hr + xi * hi) * scale
        lhs[here, :, 128:256] = (xr * hi - xi * hr) * scale
    back = jnp.dot(
        lhs[pl.ds(0, NK)].reshape(NK * 8, 256), across[...], precision=HIGHEST, preferred_element_type=jnp.float32
    )
    spec[pl.ds(0, NK)] = back.reshape(NK, 8, 256)
    for at in range(0, NK, CHUNK):
        here = pl.ds(at, CHUNK)
        c, s = twist[0, here], twist[1, here]
        re, im = spec[here, :, 0:128], spec[here, :, 128:256]
        spec[here, :, 0:128] = re * c - im * s
        spec[here, :, 128:256] = re * s + im * c
    for i in (24, 28):
        spec[i] = spec[i] * 0.5
    rows_inverse(spec, part, out_ref)


def exchange_kernel(
    n,
    x_ref, index_hbm, damp_hbm, wave_ref, across_ref, twist_ref,
    o_ref,
    index_ref, damp_ref, raw, own, note, bank, taps, floors, across, twist, part, lhs, spec,
    send, recv, note_send, note_recv, wave_send, wave_recv, fours_send, fours_recv, pass_sem, own_sem, table_sem, word,
):
    me = lax.axis_index("traces")
    chips = n // 2
    z, core = me // 2, me % 2
    group = lax.axis_index("groups")
    half = group % 2

    def place_of(z, core):
        return core * chips + (z % 4) * (chips // 4) + z // 4

    mine = place_of(z, core)

    def offset(k):
        far = (k + n - 8) // n
        m = k // 2
        sign = 1 - 2 * (k % 2)
        near_dz = (m + 1) // 2 + (chips // 2 - 2) * (m // 3)
        one = ((m + 1) // 2) % 2
        near_dc = one * (m // 2) + (1 - one) * (k % 2)
        dz = sign * (far * (chips // 2 + 1 - k // 4) + (1 - far) * near_dz)
        dc = far * (m % 2) + (1 - far) * near_dc
        return dz, dc

    def target(k):
        dz, dc = offset(k)
        return ((z + dz + chips) % chips) * 2 + (core + dc) % 2

    def source(k):
        dz, dc = offset(k)
        return (z - dz + chips) % chips, (core + dc) % 2

    def eight_rows(i):
        return pl.ds(pl.multiple_of(i * 8, 8), 8)

    def raw_copy(k):
        t = target(k)
        return pltpu.make_async_remote_copy(
            src_ref=x_ref.at[eight_rows(t)], dst_ref=raw.at[k], send_sem=send.at[k], recv_sem=recv.at[k],
            device_id={"traces": t}, device_id_type=MESH,
        )

    def late_copy(k):
        return pltpu.make_async_remote_copy(
            src_ref=o_ref.at[k + LATE], dst_ref=o_ref.at[me], send_sem=send.at[k], recv_sem=recv.at[k],
            device_id={"traces": target(k)}, device_id_type=MESH,
        )

    def late_input(k):
        return pltpu.make_async_copy(x_ref.at[eight_rows(target(k))], raw.at[k], own_sem.at[k - (n - LATE)])

    def note_copy(k):
        t = target(k)
        return pltpu.make_async_remote_copy(
            src_ref=own.at[t], dst_ref=note.at[mine], send_sem=note_send.at[k], recv_sem=note_recv.at[k],
            device_id={"traces": t}, device_id_type=MESH,
        )

    own_taps = wave_ref.at[:, pl.ds(pl.multiple_of(half * 128, 128), 128)]

    def wave_copy(j):
        return pltpu.make_async_remote_copy(
            src_ref=own_taps, dst_ref=bank.at[half, core, z % 4, z // 4], send_sem=wave_send.at[j], recv_sem=wave_recv.at[j],
            device_id={"traces": ((z + 4 * j) % chips) * 2 + core}, device_id_type=MESH,
        )

    def fours_copy(j):
        away = (0, 1, 2, chips - 1)[j]
        here = bank.at[half, core, z % 4]
        return pltpu.make_async_remote_copy(
            src_ref=here, dst_ref=here, send_sem=fours_send.at[j], recv_sem=fours_recv.at[j],
            device_id={"traces": ((z + away) % chips) * 2 + core}, device_id_type=MESH,
        )

    def pass_copy():
        return pltpu.make_async_remote_copy(
            src_ref=bank.at[half, core], dst_ref=bank.at[half, core], send_sem=pass_sem.at[0], recv_sem=pass_sem.at[1],
            device_id={"traces": z * 2 + 1 - core}, device_id_type=MESH,
        )

    def cross_copy():
        return pltpu.make_async_remote_copy(
            src_ref=bank.at[half], dst_ref=bank.at[half], send_sem=pass_sem.at[2], recv_sem=pass_sem.at[3],
            device_id={"groups": group + 1 - 2 * half, "traces": me}, device_id_type=MESH,
        )

    right = lax.rem(z + 1, chips) * 2
    left = lax.rem(z + (chips - 1), chips) * 2
    barrier = pltpu.get_barrier_semaphore()
    for there in (right + core, left + core, right + 1 - core, left + 1 - core, z * 2 + 1 - core):
        pl.semaphore_signal(barrier, inc=1, device_id={"traces": there}, device_id_type=MESH)
    other = {"groups": group + 1 - 2 * half, "traces": me}
    pl.semaphore_signal(barrier, inc=1, device_id=other, device_id_type=MESH)
    pl.semaphore_wait(barrier, 6)

    def tell(side):
        there = (right if side == 0 else left) + core
        pl.semaphore_signal(word.at[side], inc=1, device_id={"traces": there}, device_id_type=MESH)

    tell(0)
    tell(1)
    for k in (2, 3, 4, 5, 1):
        raw_copy(k).start()
    small = [
        pltpu.make_async_copy(index_hbm, index_ref, table_sem.at[2]),
        pltpu.make_async_copy(damp_hbm, damp_ref, table_sem.at[3]),
        pltpu.make_async_copy(own_taps, bank.at[half, core, z % 4, z // 4], table_sem.at[4]),
    ]
    for copy in small:
        copy.start()

    def hear(_, __):
        for side in (0, 1):
            pl.semaphore_wait(word.at[side], 1)
            tell(side)
        return 0

    lax.fori_loop(0, chips // 2 - 2, hear, 0)
    for side in (0, 1):
        pl.semaphore_wait(word.at[side], 1)

    def start_note(k, _):
        note_copy(k).start()
        return 0

    def start_raw(k, _):
        raw_copy(k).start()
        return 0

    def start_late(k, _):
        late_copy(k).start()
        return 0

    def start_input(k, _):
        late_input(k).start()
        return 0

    def wait_note(k, _):
        note_copy(k).wait()
        return 0

    def wait_input(k, _):
        late_input(k).wait()
        return 0

    for j in range(1, chips // 4):
        wave_copy(j).start()
    for k in (8, 9):
        raw_copy(k).start()
    own_copy = pltpu.make_async_copy(x_ref.at[eight_rows(me)], raw.at[0], own_sem.at[LATE])
    own_copy.start()
    across_copy = pltpu.make_async_copy(across_ref, across, table_sem.at[0])
    across_copy.start()
    twist_copy = pltpu.make_async_copy(twist_ref, twist, table_sem.at[1])
    twist_copy.start()
    lax.fori_loop(n - LATE, n, start_input, 0)
    for copy in small:
        copy.wait()
    lane = lax.broadcasted_iota(jnp.int32, (1, 128), 1)
    damp = jnp.zeros((1, 128), jnp.float32)
    for i in range(8):
        damp = jnp.where(lane == 8 + i, damp_ref[i], damp)

    def fill(e, _):
        row = damp
        for i in range(8):
            row = jnp.where(lane == i, index_ref[e * 8 + i].astype(jnp.float32), row)
        own[e] = row
        return 0

    lax.fori_loop(0, n, fill, 0)
    note[mine] = own[me]
    for j in range(1, chips // 4):
        wave_copy(j).wait()
    for j in (1, 2, 3):
        fours_copy(j).start()
    lax.fori_loop(1, n, start_note, 0)
    lax.fori_loop(6, 8, start_raw, 0)
    lax.fori_loop(10, n - LATE, start_raw, 0)
    own_copy.wait()
    across_copy.wait()
    twist_copy.wait()
    lax.fori_loop(n - LATE, n, wait_input, 0)
    for j in (1, 2, 3):
        fours_copy(j).wait()
    pass_copy().start()
    lax.fori_loop(1, n, wait_note, 0)
    pass_copy().wait()
    cross_copy().start()
    cross_copy().wait()

    lanes = lax.broadcasted_iota(jnp.int32, (n, 8, 128), 2)
    place = lax.broadcasted_iota(jnp.int32, (n, 8, 128), 1)

    def spread(notes, at):
        return jnp.sum(jnp.where(lanes == place + at, notes, 0.0), axis=2, keepdims=True).reshape(8 * n, 1)

    damping = spread(note[...], 8)
    every = jnp.concatenate([bank[0].reshape(8 * n, 128), bank[1].reshape(8 * n, 128)], axis=1)
    level = jnp.sum(every * every, axis=1, keepdims=True)
    water = jnp.broadcast_to(damping * (level + 1e-6), (8 * n, 128))
    slot = lax.broadcasted_iota(jnp.int32, (8 * n, 8 * n), 1)
    chip = ((slot // 8) % (chips // 4)) * 4 + (slot // (2 * chips)) % 4
    ids = chip * 16 + (slot // (8 * chips)) * 8 + slot % 8
    for half, notes in enumerate((note, own)):
        pick = jnp.where(spread(notes[...], 0) == ids.astype(jnp.float32), 1.0, 0.0).astype(jnp.float32)
        here = pl.ds(half * n, n)
        taps[here] = jnp.dot(pick, every, precision=HIGHEST, preferred_element_type=jnp.float32).reshape(n, 8, 256)
        floors[here] = jnp.dot(pick, water, precision=HIGHEST, preferred_element_type=jnp.float32).reshape(n, 8, 128)

    def block(i, _):
        k = (i + n - LATE) % n
        raws = (i + n - LATE) // n
        sz, sc = source(k)

        @pl.when(i > LATE)
        def _():
            raw_copy(k).wait_recv()

        @pl.when(i == LATE + 1)
        def _():
            lax.fori_loop(n - LATE, n, start_late, 0)

        out = raws * (sz * 2 + sc) + (1 - raws) * (n + i)
        p = raws * place_of(sz, sc) + (1 - raws) * (n + target(k))
        deconvolve(raw.at[k], o_ref.at[out], taps.at[p], floors.at[p], across, twist, part, lhs, spec)
        return 0

    lax.fori_loop(0, n, block, 0)

    def finish_raw(k, _):
        raw_copy(k).wait_send()
        return 0

    def finish_late(k, _):
        late_copy(k).wait()
        return 0

    lax.fori_loop(1, n - LATE, finish_raw, 0)
    lax.fori_loop(n - LATE, n, finish_late, 0)


def exchange(n, x, index, damp, wave, across, twist):
    rows, length = x.shape
    hbm = pl.BlockSpec(memory_space=pltpu.HBM)
    f32 = jnp.float32
    dma = pltpu.SemaphoreType.DMA
    return pl.pallas_call(
        functools.partial(exchange_kernel, n),
        out_shape=jax.ShapeDtypeStruct((n + LATE, 8 * PITCH, 128), f32),
        in_specs=[hbm] * 6,
        out_specs=pl.BlockSpec(memory_space=pltpu.VMEM),
        scratch_shapes=[
            pltpu.SMEM(index.shape, jnp.int32),
            pltpu.SMEM(damp.shape, f32),
            pltpu.VMEM((n, 8, length), f32),
            pltpu.VMEM((n, 1, 128), f32),
            pltpu.VMEM((n, 1, 128), f32),
            pltpu.VMEM((2, 2, 4, n // 8, 8, 128), f32),
            pltpu.VMEM((2 * n, 8, 256), f32),
            pltpu.VMEM((2 * n, 8, 128), f32),
            pltpu.VMEM(across.shape, f32),
            pltpu.VMEM(twist.shape, f32),
            pltpu.VMEM((8, 8, 8, 128), f32),
            pltpu.VMEM((2 * NK, 8, 256), f32),
            pltpu.VMEM((2 * NK, 8, 256), f32),
            dma((n,)), dma((n,)), dma((n,)), dma((n,)), dma((n // 8,)), dma((n // 8,)), dma((4,)), dma((4,)), dma((4,)),
            dma((LATE + 1,)), dma((5,)), pltpu.SemaphoreType.REGULAR((2,)),
        ],
        compiler_params=pltpu.CompilerParams(collective_id=0, has_side_effects=True, vmem_limit_bytes=VMEM_LIMIT),
    )(*(pltpu.with_memory_space_constraint(a, pltpu.HBM) for a in (x, index, damp, wave, across, twist)))


def reorder_kernel(n, order_ref, x_ref, o_ref, *scratch):
    *helds, lined, out_sem = scratch
    rows = o_ref.shape[0]
    tiles = rows // 8

    def out_copy(t):
        here = pl.ds(pl.multiple_of(t * 8, 8), 8)
        return pltpu.make_async_copy(lined.at[here], o_ref.at[here], out_sem.at[t])

    def line_up(g, _):
        for u, held in enumerate(helds):
            t = g * len(helds) + u
            for i in range(8):
                p = order_ref[t * 8 + i]
                held[pl.ds(i * PITCH, 64), :] = x_ref[p % n, pl.ds((p // n) * PITCH, 64), :]
        for u, held in enumerate(helds):
            t = g * len(helds) + u
            here = pl.ds(pl.multiple_of(t * 8, 8), 8)
            for i in range(64):
                lined[here, pl.ds(i * 128, 128)] = held[pl.ds(i, 8, stride=PITCH), :]
            out_copy(t).start()
        return 0

    lax.fori_loop(0, tiles // len(helds), line_up, 0)

    def finish(t, _):
        out_copy(t).wait()
        return 0

    lax.fori_loop(0, tiles, finish, 0)


def reorder(n, order, x):
    rows, length = order.shape[0], 8192
    return pl.pallas_call(
        functools.partial(reorder_kernel, n),
        out_shape=jax.ShapeDtypeStruct((rows, length), x.dtype),
        in_specs=[pl.BlockSpec(memory_space=pltpu.SMEM), pl.BlockSpec(memory_space=pltpu.VMEM)],
        out_specs=pl.BlockSpec(memory_space=pl.ANY),
        scratch_shapes=[
            *[pltpu.VMEM((8 * PITCH, 128), x.dtype)] * 4,
            pltpu.VMEM((rows, length), x.dtype),
            pltpu.SemaphoreType.DMA((rows // 8,)),
        ],
        compiler_params=pltpu.CompilerParams(vmem_limit_bytes=VMEM_LIMIT),
    )(order, x)


def solution(mesh):
    n = mesh.shape["traces"]
    across, twist = tables()

    def local(raw_traces, filter_index, channel_order, wavelets, damping):
        moved = exchange(n, raw_traces, filter_index, damping, wavelets, jnp.asarray(across), jnp.asarray(twist))
        return reorder(n, channel_order, moved)

    placed = (
        P(("groups", "traces"), None),
        P(("groups", "traces")),
        P("groups"),
        P("traces", None),
        P("traces"),
    )
    return jax.shard_map(
        local, mesh=mesh, in_specs=placed, out_specs=P(("groups", "traces"), None), check_vma=False
    )
```

```python
import functools
import math

import jax
import jax.numpy as jnp
import numpy as np
from jax import lax
from jax.experimental import pallas as pl
from jax.experimental.pallas import tpu as pltpu
from jax.sharding import PartitionSpec as P

MESH = pl.DeviceIdType.MESH
HIGHEST = lax.Precision.HIGHEST
HALF_ROOT = math.sqrt(0.5)

KEPT = [a + 8 * b for a in (1, 2, 3) for b in range(8)] + [8 * b for b in range(5)] + [4 + 8 * b for b in range(4)]
NK = len(KEPT)
CHUNK = 11
PITCH = 65
VMEM_LIMIT = 34 * 2**20
LATE = 8


def tables():
    q = np.arange(128)
    turn = 2.0 * np.pi * (np.outer(q, q) % 128) / 128
    c, s = np.cos(turn), np.sin(turn)
    across = np.block([[c, -s], [s, c]]).astype(np.float32)
    twist = []
    for shift in (0, 128):
        angle = 2.0 * np.pi * (np.outer(KEPT, q + shift) % 8192) / 8192
        twist += [np.cos(angle), -np.sin(angle)]
    twist = np.stack(twist).astype(np.float32)
    return across, np.ascontiguousarray(np.broadcast_to(twist[:, :, None, :], (4, NK, 8, 128)))


def rotate(re, im, step):
    step %= 64
    if step == 0:
        return re, im
    c, s = math.cos(2 * math.pi * step / 64), math.sin(2 * math.pi * step / 64)
    return re * c + im * s, im * c - re * s


def four(x):
    (ar, ai), (br, bi), (cr, ci), (dr, di) = x
    sr, si, tr, ti = ar + cr, ai + ci, ar - cr, ai - ci
    ur, ui, vr, vi = br + dr, bi + di, br - dr, bi - di
    return [(sr + ur, si + ui), (tr + vi, ti - vr), (sr - ur, si - ui), (tr - vi, ti + vr)]


def eight(x):
    e, o = four(x[0::2]), four(x[1::2])
    r = HALF_ROOT
    w = [
        o[0],
        (r * (o[1][0] + o[1][1]), r * (o[1][1] - o[1][0])),
        (o[2][1], -o[2][0]),
        (r * (o[3][1] - o[3][0]), -r * (o[3][0] + o[3][1])),
    ]
    low = [(e[k][0] + w[k][0], e[k][1] + w[k][1]) for k in range(4)]
    high = [(e[k][0] - w[k][0], e[k][1] - w[k][1]) for k in range(4)]
    return low + high


def eight_real(x):
    s, t, u, v = x[0] + x[4], x[0] - x[4], x[2] + x[6], x[2] - x[6]
    s2, t2, u2, v2 = x[1] + x[5], x[1] - x[5], x[3] + x[7], x[3] - x[7]
    e0, o0 = s + u, s2 + u2
    wr, wi = HALF_ROOT * (t2 - v2), -HALF_ROOT * (t2 + v2)
    return [
        (e0 + o0, None),
        (t + wr, wi - v),
        (s - u, u2 - s2),
        (t - wr, v + wi),
        (e0 - o0, None),
    ]


def total(terms):
    terms = list(terms)
    while len(terms) > 1:
        terms = [terms[i] + terms[i + 1] if i + 1 < len(terms) else terms[i] for i in range(0, len(terms), 2)]
    return terms[0]


def rows_forward(x_ref, part, lhs):
    for b in range(8):
        v = eight_real([x_ref[:, pl.ds((8 * a + b) * 128, 128)] for a in range(8)])
        part[b, 0] = v[0][0]
        part[b, 7] = v[4][0]
        for k in (1, 2, 3):
            re, im = rotate(v[k][0], v[k][1], b * k)
            part[b, 2 * k - 1] = re
            part[b, 2 * k] = im
    for k in (1, 2, 3):
        out = eight([(part[b, 2 * k - 1], part[b, 2 * k]) for b in range(8)])
        for b in range(8):
            lhs[8 * (k - 1) + b, :, 0:128] = out[b][0]
            lhs[8 * (k - 1) + b, :, 128:256] = out[b][1]
    out = eight_real([part[b, 0] for b in range(8)])
    for b in range(5):
        lhs[24 + b, :, 0:128] = out[b][0]
        lhs[24 + b, :, 128:256] = jnp.zeros((8, 128), jnp.float32) if out[b][1] is None else out[b][1]
    real = [part[b, 7] for b in range(8)]
    for j in range(4):
        angles = [2 * math.pi * b * (2 * j + 1) / 16 for b in range(8)]
        lhs[29 + j, :, 0:128] = total(real[b] * math.cos(angles[b]) for b in range(8))
        lhs[29 + j, :, 128:256] = total(real[b] * -math.sin(angles[b]) for b in range(1, 8))


def rows_inverse(spec, part, out_ref):
    def at(i):
        return spec[i, :, 0:128], spec[i, :, 128:256]

    for k in (1, 2, 3):
        out = eight([at(8 * (k - 1) + b) for b in range(8)])
        for b in range(8):
            re, im = rotate(out[b][0], out[b][1], b * k)
            part[b, 2 * k - 1] = re
            part[b, 2 * k] = im
    zero = [at(24 + j) for j in range(5)]
    four_ = [at(29 + j) for j in range(4)]
    for b in range(8):
        terms = [zero[0][0], zero[4][0] if b % 2 == 0 else -zero[4][0]]
        for j in (1, 2, 3):
            terms.append(rotate(*zero[j], 8 * b * j)[0])
        part[b, 0] = total(terms)
        part[b, 7] = total(rotate(*four_[j], b * (4 + 8 * j))[0] for j in range(4))
    for b in range(8):
        e0, p1, m1, p2, m2, p3, m3, e4 = (part[b, i] for i in range(8))
        g0, g1 = e0 + e4, e0 - e4
        for a, base, turn in (
            (0, g0 + p2, p1 + p3),
            (2, g0 - p2, m1 - m3),
            (1, g1 + m2, HALF_ROOT * ((p1 + m1) + (m3 - p3))),
            (3, g1 - m2, HALF_ROOT * ((m1 - p1) + (p3 + m3))),
        ):
            out_ref[pl.ds(8 * a + b, 8, stride=PITCH), :] = base + turn
            out_ref[pl.ds(8 * (a + 4) + b, 8, stride=PITCH), :] = base - turn


def deconvolve(x_ref, out_ref, tap_ref, floor_ref, across, twist, part, lhs, spec):
    rows_forward(x_ref, part, lhs)
    h0, h1 = tap_ref[:, 0:128][None], tap_ref[:, 128:256][None]
    for at in range(0, NK, CHUNK):
        here = pl.ds(at, CHUNK)
        c, s = twist[0, here], twist[1, here]
        re, im = lhs[here, :, 0:128], lhs[here, :, 128:256]
        lhs[here, :, 0:128] = re * c - im * s
        lhs[here, :, 128:256] = re * s + im * c
        there = pl.ds(NK + at, CHUNK)
        lhs[there, :, 0:128] = h0 * c + h1 * twist[2, here]
        lhs[there, :, 128:256] = h0 * s + h1 * twist[3, here]
    both = jnp.dot(lhs[...].reshape(2 * NK * 8, 256), across[...], precision=HIGHEST, preferred_element_type=jnp.float32)
    spec[...] = both.reshape(2 * NK, 8, 256)
    floor = floor_ref[...][None]
    for at in range(0, NK, CHUNK):
        here, there = pl.ds(at, CHUNK), pl.ds(NK + at, CHUNK)
        xr, xi = spec[here, :, 0:128], spec[here, :, 128:256]
        hr, hi = spec[there, :, 0:128], spec[there, :, 128:256]
        scale = (2.0 / 8192) / ((hr * hr + hi * hi) + floor)
        lhs[here, :, 0:128] = (xr * hr + xi * hi) * scale
        lhs[here, :, 128:256] = (xr * hi - xi * hr) * scale
    back = jnp.dot(
        lhs[pl.ds(0, NK)].reshape(NK * 8, 256), across[...], precision=HIGHEST, preferred_element_type=jnp.float32
    )
    spec[pl.ds(0, NK)] = back.reshape(NK, 8, 256)
    for at in range(0, NK, CHUNK):
        here = pl.ds(at, CHUNK)
        c, s = twist[0, here], twist[1, here]
        re, im = spec[here, :, 0:128], spec[here, :, 128:256]
        spec[here, :, 0:128] = re * c - im * s
        spec[here, :, 128:256] = re * s + im * c
    for i in (24, 28):
        spec[i] = spec[i] * 0.5
    rows_inverse(spec, part, out_ref)


def exchange_kernel(
    n,
    x_ref, index_hbm, damp_hbm, wave_ref, across_ref, twist_ref,
    o_ref,
    index_ref, damp_ref, raw, own, note, bank, taps, floors, across, twist, part, lhs, spec,
    send, recv, note_send, note_recv, wave_send, wave_recv, fours_send, fours_recv, pass_sem, own_sem, table_sem, word,
):
    me = lax.axis_index("traces")
    chips = n // 2
    z, core = me // 2, me % 2
    group = lax.axis_index("groups")
    half = group % 2

    def place_of(z, core):
        return core * chips + (z % 4) * (chips // 4) + z // 4

    mine = place_of(z, core)

    def offset(k):
        far = (k + n - 8) // n
        m = k // 2
        sign = 1 - 2 * (k % 2)
        near_dz = (m + 1) // 2 + (chips // 2 - 2) * (m // 3)
        one = ((m + 1) // 2) % 2
        near_dc = one * (m // 2) + (1 - one) * (k % 2)
        dz = sign * (far * (chips // 2 + 1 - k // 4) + (1 - far) * near_dz)
        dc = far * (m % 2) + (1 - far) * near_dc
        return dz, dc

    def target(k):
        dz, dc = offset(k)
        return ((z + dz + chips) % chips) * 2 + (core + dc) % 2

    def source(k):
        dz, dc = offset(k)
        return (z - dz + chips) % chips, (core + dc) % 2

    def eight_rows(i):
        return pl.ds(pl.multiple_of(i * 8, 8), 8)

    def raw_copy(k):
        t = target(k)
        return pltpu.make_async_remote_copy(
            src_ref=x_ref.at[eight_rows(t)], dst_ref=raw.at[k], send_sem=send.at[k], recv_sem=recv.at[k],
            device_id={"traces": t}, device_id_type=MESH,
        )

    def late_copy(k, at, size):
        here = pl.ds(at, size)
        return pltpu.make_async_remote_copy(
            src_ref=o_ref.at[k + LATE, here], dst_ref=o_ref.at[me, here], send_sem=send.at[k], recv_sem=recv.at[k],
            device_id={"traces": target(k)}, device_id_type=MESH,
        )

    def late_input(k):
        return pltpu.make_async_copy(x_ref.at[eight_rows(target(k))], raw.at[k], own_sem.at[k - (n - LATE)])

    def note_copy(k):
        t = target(k)
        return pltpu.make_async_remote_copy(
            src_ref=own.at[t], dst_ref=note.at[mine], send_sem=note_send.at[k], recv_sem=note_recv.at[k],
            device_id={"traces": t}, device_id_type=MESH,
        )

    own_taps = wave_ref.at[:, pl.ds(pl.multiple_of(half * 128, 128), 128)]

    def wave_copy(j):
        return pltpu.make_async_remote_copy(
            src_ref=own_taps, dst_ref=bank.at[half, core, z % 4, z // 4], send_sem=wave_send.at[j], recv_sem=wave_recv.at[j],
            device_id={"traces": ((z + 4 * j) % chips) * 2 + core}, device_id_type=MESH,
        )

    def fours_copy(j):
        away = (0, 1, 2, chips - 1)[j]
        here = bank.at[half, core, z % 4]
        return pltpu.make_async_remote_copy(
            src_ref=here, dst_ref=here, send_sem=fours_send.at[j], recv_sem=fours_recv.at[j],
            device_id={"traces": ((z + away) % chips) * 2 + core}, device_id_type=MESH,
        )

    def pass_copy():
        return pltpu.make_async_remote_copy(
            src_ref=bank.at[half, core], dst_ref=bank.at[half, core], send_sem=pass_sem.at[0], recv_sem=pass_sem.at[1],
            device_id={"traces": z * 2 + 1 - core}, device_id_type=MESH,
        )

    def cross_copy():
        return pltpu.make_async_remote_copy(
            src_ref=bank.at[half], dst_ref=bank.at[half], send_sem=pass_sem.at[2], recv_sem=pass_sem.at[3],
            device_id={"groups": group + 1 - 2 * half, "traces": me}, device_id_type=MESH,
        )

    right = lax.rem(z + 1, chips) * 2
    left = lax.rem(z + (chips - 1), chips) * 2
    barrier = pltpu.get_barrier_semaphore()
    for there in (right + core, left + core, right + 1 - core, left + 1 - core, z * 2 + 1 - core):
        pl.semaphore_signal(barrier, inc=1, device_id={"traces": there}, device_id_type=MESH)
    other = {"groups": group + 1 - 2 * half, "traces": me}
    pl.semaphore_signal(barrier, inc=1, device_id=other, device_id_type=MESH)
    pl.semaphore_wait(barrier, 6)

    def tell(side):
        there = (right if side == 0 else left) + core
        pl.semaphore_signal(word.at[side], inc=1, device_id={"traces": there}, device_id_type=MESH)

    tell(0)
    tell(1)
    for k in (2, 3, 4, 5, 1):
        raw_copy(k).start()
    small = [
        pltpu.make_async_copy(index_hbm, index_ref, table_sem.at[2]),
        pltpu.make_async_copy(damp_hbm, damp_ref, table_sem.at[3]),
        pltpu.make_async_copy(own_taps, bank.at[half, core, z % 4, z // 4], table_sem.at[4]),
    ]
    for copy in small:
        copy.start()

    def hear(_, __):
        for side in (0, 1):
            pl.semaphore_wait(word.at[side], 1)
            tell(side)
        return 0

    lax.fori_loop(0, chips // 2 - 2, hear, 0)
    for side in (0, 1):
        pl.semaphore_wait(word.at[side], 1)

    def start_note(k, _):
        note_copy(k).start()
        return 0

    def start_raw(k, _):
        raw_copy(k).start()
        return 0

    def start_late(k, _):
        for i in range(8):
            late_copy(k, i * PITCH, 64).start()
        return 0

    def start_input(k, _):
        late_input(k).start()
        return 0

    def wait_note(k, _):
        note_copy(k).wait()
        return 0

    def wait_input(k, _):
        late_input(k).wait()
        return 0

    for j in range(1, chips // 4):
        wave_copy(j).start()
    for k in (8, 9):
        raw_copy(k).start()
    own_copy = pltpu.make_async_copy(x_ref.at[eight_rows(me)], raw.at[0], own_sem.at[LATE])
    own_copy.start()
    across_copy = pltpu.make_async_copy(across_ref, across, table_sem.at[0])
    across_copy.start()
    twist_copy = pltpu.make_async_copy(twist_ref, twist, table_sem.at[1])
    twist_copy.start()
    lax.fori_loop(n - LATE, n, start_input, 0)
    for copy in small:
        copy.wait()
    lane = lax.broadcasted_iota(jnp.int32, (1, 128), 1)
    damp = jnp.zeros((1, 128), jnp.float32)
    for i in range(8):
        damp = jnp.where(lane == 8 + i, damp_ref[i], damp)

    def fill(e, _):
        row = damp
        for i in range(8):
            row = jnp.where(lane == i, index_ref[e * 8 + i].astype(jnp.float32), row)
        own[e] = row
        return 0

    lax.fori_loop(0, n, fill, 0)
    note[mine] = own[me]
    for j in range(1, chips // 4):
        wave_copy(j).wait()
    for j in (1, 2, 3):
        fours_copy(j).start()
    lax.fori_loop(1, n, start_note, 0)
    lax.fori_loop(6, 8, start_raw, 0)
    lax.fori_loop(10, n - LATE, start_raw, 0)
    own_copy.wait()
    across_copy.wait()
    twist_copy.wait()
    lax.fori_loop(n - LATE, n, wait_input, 0)
    for j in (1, 2, 3):
        fours_copy(j).wait()
    pass_copy().start()
    lax.fori_loop(1, n, wait_note, 0)
    pass_copy().wait()
    cross_copy().start()
    cross_copy().wait()

    lanes = lax.broadcasted_iota(jnp.int32, (n, 8, 128), 2)
    place = lax.broadcasted_iota(jnp.int32, (n, 8, 128), 1)

    def spread(notes, at):
        return jnp.sum(jnp.where(lanes == place + at, notes, 0.0), axis=2, keepdims=True).reshape(8 * n, 1)

    damping = spread(note[...], 8)
    every = jnp.concatenate([bank[0].reshape(8 * n, 128), bank[1].reshape(8 * n, 128)], axis=1)
    level = jnp.sum(every * every, axis=1, keepdims=True)
    water = jnp.broadcast_to(damping * (level + 1e-6), (8 * n, 128))
    slot = lax.broadcasted_iota(jnp.int32, (8 * n, 8 * n), 1)
    chip = ((slot // 8) % (chips // 4)) * 4 + (slot // (2 * chips)) % 4
    ids = chip * 16 + (slot // (8 * chips)) * 8 + slot % 8
    for half, notes in enumerate((note, own)):
        pick = jnp.where(spread(notes[...], 0) == ids.astype(jnp.float32), 1.0, 0.0).astype(jnp.float32)
        here = pl.ds(half * n, n)
        taps[here] = jnp.dot(pick, every, precision=HIGHEST, preferred_element_type=jnp.float32).reshape(n, 8, 256)
        floors[here] = jnp.dot(pick, water, precision=HIGHEST, preferred_element_type=jnp.float32).reshape(n, 8, 128)

    def block(i, _):
        k = (i + n - LATE) % n
        raws = (i + n - LATE) // n
        sz, sc = source(k)

        @pl.when(i > LATE)
        def _():
            raw_copy(k).wait_recv()

        @pl.when(i == LATE + 1)
        def _():
            lax.fori_loop(n - LATE, n, start_late, 0)

        out = raws * (sz * 2 + sc) + (1 - raws) * (n + i)
        p = raws * place_of(sz, sc) + (1 - raws) * (n + target(k))
        deconvolve(raw.at[k], o_ref.at[out], taps.at[p], floors.at[p], across, twist, part, lhs, spec)
        return 0

    lax.fori_loop(0, n, block, 0)

    def finish_raw(k, _):
        raw_copy(k).wait_send()
        return 0

    def finish_late(k, _):
        late_copy(k, 0, 512).wait()
        return 0

    lax.fori_loop(1, n - LATE, finish_raw, 0)
    lax.fori_loop(n - LATE, n, finish_late, 0)


def exchange(n, x, index, damp, wave, across, twist):
    rows, length = x.shape
    hbm = pl.BlockSpec(memory_space=pltpu.HBM)
    f32 = jnp.float32
    dma = pltpu.SemaphoreType.DMA
    return pl.pallas_call(
        functools.partial(exchange_kernel, n),
        out_shape=jax.ShapeDtypeStruct((n + LATE, 8 * PITCH, 128), f32),
        in_specs=[hbm] * 6,
        out_specs=pl.BlockSpec(memory_space=pltpu.VMEM),
        scratch_shapes=[
            pltpu.SMEM(index.shape, jnp.int32),
            pltpu.SMEM(damp.shape, f32),
            pltpu.VMEM((n, 8, length), f32),
            pltpu.VMEM((n, 1, 128), f32),
            pltpu.VMEM((n, 1, 128), f32),
            pltpu.VMEM((2, 2, 4, n // 8, 8, 128), f32),
            pltpu.VMEM((2 * n, 8, 256), f32),
            pltpu.VMEM((2 * n, 8, 128), f32),
            pltpu.VMEM(across.shape, f32),
            pltpu.VMEM(twist.shape, f32),
            pltpu.VMEM((8, 8, 8, 128), f32),
            pltpu.VMEM((2 * NK, 8, 256), f32),
            pltpu.VMEM((2 * NK, 8, 256), f32),
            dma((n,)), dma((n,)), dma((n,)), dma((n,)), dma((n // 8,)), dma((n // 8,)), dma((4,)), dma((4,)), dma((4,)),
            dma((LATE + 1,)), dma((5,)), pltpu.SemaphoreType.REGULAR((2,)),
        ],
        compiler_params=pltpu.CompilerParams(collective_id=0, has_side_effects=True, vmem_limit_bytes=VMEM_LIMIT),
    )(*(pltpu.with_memory_space_constraint(a, pltpu.HBM) for a in (x, index, damp, wave, across, twist)))


def reorder_kernel(n, order_ref, x_ref, o_ref, *scratch):
    *helds, lined, out_sem = scratch
    rows = o_ref.shape[0]
    tiles = rows // 8

    def out_copy(t):
        here = pl.ds(pl.multiple_of(t * 8, 8), 8)
        return pltpu.make_async_copy(lined.at[here], o_ref.at[here], out_sem)

    def line_up(g, _):
        for u, held in enumerate(helds):
            t = g * len(helds) + u
            for i in range(8):
                p = order_ref[t * 8 + i]
                held[pl.ds(i * PITCH, 64), :] = x_ref[p % n, pl.ds((p // n) * PITCH, 64), :]
        for u, held in enumerate(helds):
            t = g * len(helds) + u
            here = pl.ds(pl.multiple_of(t * 8, 8), 8)
            for i in range(64):
                lined[here, pl.ds(i * 128, 128)] = held[pl.ds(i, 8, stride=PITCH), :]
            out_copy(t).start()
        return 0

    lax.fori_loop(0, tiles // len(helds), line_up, 0)

    pltpu.make_async_copy(lined, o_ref, out_sem).wait()


def reorder(n, order, x):
    rows, length = order.shape[0], 8192
    return pl.pallas_call(
        functools.partial(reorder_kernel, n),
        out_shape=jax.ShapeDtypeStruct((rows, length), x.dtype),
        in_specs=[pl.BlockSpec(memory_space=pltpu.SMEM), pl.BlockSpec(memory_space=pltpu.VMEM)],
        out_specs=pl.BlockSpec(memory_space=pl.ANY),
        scratch_shapes=[
            *[pltpu.VMEM((8 * PITCH, 128), x.dtype)] * 4,
            pltpu.VMEM((rows, length), x.dtype),
            pltpu.SemaphoreType.DMA,
        ],
        compiler_params=pltpu.CompilerParams(vmem_limit_bytes=VMEM_LIMIT),
    )(order, x)


def solution(mesh):
    n = mesh.shape["traces"]
    across, twist = tables()

    def local(raw_traces, filter_index, channel_order, wavelets, damping):
        moved = exchange(n, raw_traces, filter_index, damping, wavelets, jnp.asarray(across), jnp.asarray(twist))
        return reorder(n, channel_order, moved)

    placed = (
        P(("groups", "traces"), None),
        P(("groups", "traces")),
        P("groups"),
        P("traces", None),
        P("traces"),
    )
    return jax.shard_map(
        local, mesh=mesh, in_specs=placed, out_specs=P(("groups", "traces"), None), check_vma=False
    )
```

```python
import functools
import math

import jax
import jax.numpy as jnp
import numpy as np
from jax import lax
from jax.experimental import pallas as pl
from jax.experimental.pallas import tpu as pltpu
from jax.sharding import PartitionSpec as P

MESH = pl.DeviceIdType.MESH
HIGHEST = lax.Precision.HIGHEST
HALF_ROOT = math.sqrt(0.5)

KEPT = [a + 8 * b for a in (1, 2, 3) for b in range(8)] + [8 * b for b in range(5)] + [4 + 8 * b for b in range(4)]
NK = len(KEPT)
CHUNK = 11
PITCH = 65
VMEM_LIMIT = 34 * 2**20
LATE = 8


def tables():
    q = np.arange(128)
    turn = 2.0 * np.pi * (np.outer(q, q) % 128) / 128
    c, s = np.cos(turn), np.sin(turn)
    across = np.block([[c, -s], [s, c]]).astype(np.float32)
    twist = []
    for shift in (0, 128):
        angle = 2.0 * np.pi * (np.outer(KEPT, q + shift) % 8192) / 8192
        twist += [np.cos(angle), -np.sin(angle)]
    twist = np.stack(twist).astype(np.float32)
    return across, np.ascontiguousarray(np.broadcast_to(twist[:, :, None, :], (4, NK, 8, 128)))


def rotate(re, im, step):
    step %= 64
    if step == 0:
        return re, im
    c, s = math.cos(2 * math.pi * step / 64), math.sin(2 * math.pi * step / 64)
    return re * c + im * s, im * c - re * s


def four(x):
    (ar, ai), (br, bi), (cr, ci), (dr, di) = x
    sr, si, tr, ti = ar + cr, ai + ci, ar - cr, ai - ci
    ur, ui, vr, vi = br + dr, bi + di, br - dr, bi - di
    return [(sr + ur, si + ui), (tr + vi, ti - vr), (sr - ur, si - ui), (tr - vi, ti + vr)]


def eight(x):
    e, o = four(x[0::2]), four(x[1::2])
    r = HALF_ROOT
    w = [
        o[0],
        (r * (o[1][0] + o[1][1]), r * (o[1][1] - o[1][0])),
        (o[2][1], -o[2][0]),
        (r * (o[3][1] - o[3][0]), -r * (o[3][0] + o[3][1])),
    ]
    low = [(e[k][0] + w[k][0], e[k][1] + w[k][1]) for k in range(4)]
    high = [(e[k][0] - w[k][0], e[k][1] - w[k][1]) for k in range(4)]
    return low + high


def eight_real(x):
    s, t, u, v = x[0] + x[4], x[0] - x[4], x[2] + x[6], x[2] - x[6]
    s2, t2, u2, v2 = x[1] + x[5], x[1] - x[5], x[3] + x[7], x[3] - x[7]
    e0, o0 = s + u, s2 + u2
    wr, wi = HALF_ROOT * (t2 - v2), -HALF_ROOT * (t2 + v2)
    return [
        (e0 + o0, None),
        (t + wr, wi - v),
        (s - u, u2 - s2),
        (t - wr, v + wi),
        (e0 - o0, None),
    ]


def total(terms):
    terms = list(terms)
    while len(terms) > 1:
        terms = [terms[i] + terms[i + 1] if i + 1 < len(terms) else terms[i] for i in range(0, len(terms), 2)]
    return terms[0]


def rows_forward(x_ref, part, lhs):
    for b in range(8):
        v = eight_real([x_ref[:, pl.ds((8 * a + b) * 128, 128)] for a in range(8)])
        part[b, 0] = v[0][0]
        part[b, 7] = v[4][0]
        for k in (1, 2, 3):
            re, im = rotate(v[k][0], v[k][1], b * k)
            part[b, 2 * k - 1] = re
            part[b, 2 * k] = im
    for k in (1, 2, 3):
        out = eight([(part[b, 2 * k - 1], part[b, 2 * k]) for b in range(8)])
        for b in range(8):
            lhs[8 * (k - 1) + b, :, 0:128] = out[b][0]
            lhs[8 * (k - 1) + b, :, 128:256] = out[b][1]
    out = eight_real([part[b, 0] for b in range(8)])
    for b in range(5):
        lhs[24 + b, :, 0:128] = out[b][0]
        lhs[24 + b, :, 128:256] = jnp.zeros((8, 128), jnp.float32) if out[b][1] is None else out[b][1]
    real = [part[b, 7] for b in range(8)]
    for j in range(4):
        angles = [2 * math.pi * b * (2 * j + 1) / 16 for b in range(8)]
        lhs[29 + j, :, 0:128] = total(real[b] * math.cos(angles[b]) for b in range(8))
        lhs[29 + j, :, 128:256] = total(real[b] * -math.sin(angles[b]) for b in range(1, 8))


def rows_inverse(spec, part, out_ref):
    def at(i):
        return spec[i, :, 0:128], spec[i, :, 128:256]

    for k in (1, 2, 3):
        out = eight([at(8 * (k - 1) + b) for b in range(8)])
        for b in range(8):
            re, im = rotate(out[b][0], out[b][1], b * k)
            part[b, 2 * k - 1] = re
            part[b, 2 * k] = im
    zero = [at(24 + j) for j in range(5)]
    four_ = [at(29 + j) for j in range(4)]
    for b in range(8):
        terms = [zero[0][0], zero[4][0] if b % 2 == 0 else -zero[4][0]]
        for j in (1, 2, 3):
            terms.append(rotate(*zero[j], 8 * b * j)[0])
        part[b, 0] = total(terms)
        part[b, 7] = total(rotate(*four_[j], b * (4 + 8 * j))[0] for j in range(4))
    for b in range(8):
        e0, p1, m1, p2, m2, p3, m3, e4 = (part[b, i] for i in range(8))
        g0, g1 = e0 + e4, e0 - e4
        for a, base, turn in (
            (0, g0 + p2, p1 + p3),
            (2, g0 - p2, m1 - m3),
            (1, g1 + m2, HALF_ROOT * ((p1 + m1) + (m3 - p3))),
            (3, g1 - m2, HALF_ROOT * ((m1 - p1) + (p3 + m3))),
        ):
            out_ref[pl.ds(8 * a + b, 8, stride=PITCH), :] = base + turn
            out_ref[pl.ds(8 * (a + 4) + b, 8, stride=PITCH), :] = base - turn


def deconvolve(x_ref, out_ref, tap_ref, floor_ref, across, twist, part, lhs, spec):
    rows_forward(x_ref, part, lhs)
    h0, h1 = tap_ref[:, 0:128][None], tap_ref[:, 128:256][None]
    for at in range(0, NK, CHUNK):
        here = pl.ds(at, CHUNK)
        c, s = twist[0, here], twist[1, here]
        re, im = lhs[here, :, 0:128], lhs[here, :, 128:256]
        lhs[here, :, 0:128] = re * c - im * s
        lhs[here, :, 128:256] = re * s + im * c
        there = pl.ds(NK + at, CHUNK)
        lhs[there, :, 0:128] = h0 * c + h1 * twist[2, here]
        lhs[there, :, 128:256] = h0 * s + h1 * twist[3, here]
    both = jnp.dot(lhs[...].reshape(2 * NK * 8, 256), across[...], precision=HIGHEST, preferred_element_type=jnp.float32)
    spec[...] = both.reshape(2 * NK, 8, 256)
    floor = floor_ref[...][None]
    for at in range(0, NK, CHUNK):
        here, there = pl.ds(at, CHUNK), pl.ds(NK + at, CHUNK)
        xr, xi = spec[here, :, 0:128], spec[here, :, 128:256]
        hr, hi = spec[there, :, 0:128], spec[there, :, 128:256]
        scale = (2.0 / 8192) / ((hr * hr + hi * hi) + floor)
        lhs[here, :, 0:128] = (xr * hr + xi * hi) * scale
        lhs[here, :, 128:256] = (xr * hi - xi * hr) * scale
    back = jnp.dot(
        lhs[pl.ds(0, NK)].reshape(NK * 8, 256), across[...], precision=HIGHEST, preferred_element_type=jnp.float32
    )
    spec[pl.ds(0, NK)] = back.reshape(NK, 8, 256)
    for at in range(0, NK, CHUNK):
        here = pl.ds(at, CHUNK)
        c, s = twist[0, here], twist[1, here]
        re, im = spec[here, :, 0:128], spec[here, :, 128:256]
        spec[here, :, 0:128] = re * c - im * s
        spec[here, :, 128:256] = re * s + im * c
    for i in (24, 28):
        spec[i] = spec[i] * 0.5
    rows_inverse(spec, part, out_ref)


def exchange_kernel(
    n,
    x_ref, index_hbm, damp_hbm, wave_ref, across_ref, twist_ref,
    o_ref,
    index_ref, damp_ref, raw, own, note, bank, taps, floors, across, twist, part, lhs, spec,
    send, recv, note_send, note_recv, wave_send, wave_recv, fours_send, fours_recv, pass_sem, own_sem, table_sem, word,
):
    me = lax.axis_index("traces")
    chips = n // 2
    z, core = me // 2, me % 2
    group = lax.axis_index("groups")
    half, pair = group % 2, (group // 2) % 2
    four = pl.ds(pl.multiple_of(pair * 4, 4), 4)

    def place_of(z, core):
        return core * chips + (z % 4) * (chips // 4) + z // 4

    mine = place_of(z, core)

    def offset(k):
        far = (k + n - 8) // n
        m = k // 2
        sign = 1 - 2 * (k % 2)
        near_dz = (m + 1) // 2 + (chips // 2 - 2) * (m // 3)
        one = ((m + 1) // 2) % 2
        near_dc = one * (m // 2) + (1 - one) * (k % 2)
        dz = sign * (far * (chips // 2 + 1 - k // 4) + (1 - far) * near_dz)
        dc = far * (m % 2) + (1 - far) * near_dc
        return dz, dc

    def target(k):
        dz, dc = offset(k)
        return ((z + dz + chips) % chips) * 2 + (core + dc) % 2

    def source(k):
        dz, dc = offset(k)
        return (z - dz + chips) % chips, (core + dc) % 2

    def eight_rows(i):
        return pl.ds(pl.multiple_of(i * 8, 8), 8)

    def raw_copy(k):
        t = target(k)
        return pltpu.make_async_remote_copy(
            src_ref=x_ref.at[eight_rows(t)], dst_ref=raw.at[k], send_sem=send.at[k], recv_sem=recv.at[k],
            device_id={"traces": t}, device_id_type=MESH,
        )

    def late_copy(k, at, size):
        here = pl.ds(at, size)
        return pltpu.make_async_remote_copy(
            src_ref=o_ref.at[k + LATE, here], dst_ref=o_ref.at[me, here], send_sem=send.at[k], recv_sem=recv.at[k],
            device_id={"traces": target(k)}, device_id_type=MESH,
        )

    def late_input(k):
        return pltpu.make_async_copy(x_ref.at[eight_rows(target(k))], raw.at[k], own_sem.at[k - (n - LATE)])

    def note_copy(k):
        t = target(k)
        return pltpu.make_async_remote_copy(
            src_ref=own.at[t], dst_ref=note.at[mine], send_sem=note_send.at[k], recv_sem=note_recv.at[k],
            device_id={"traces": t}, device_id_type=MESH,
        )

    own_taps = wave_ref.at[four, pl.ds(pl.multiple_of(half * 128, 128), 128)]

    def wave_copy(j):
        return pltpu.make_async_remote_copy(
            src_ref=own_taps, dst_ref=bank.at[half, core, z % 4, z // 4, four], send_sem=wave_send.at[j], recv_sem=wave_recv.at[j],
            device_id={"traces": ((z + 4 * j) % chips) * 2 + core}, device_id_type=MESH,
        )

    def fours_copy(j):
        away = (0, 1, 2, chips - 1)[j]
        here = bank.at[half, core, z % 4, :, four]
        return pltpu.make_async_remote_copy(
            src_ref=here, dst_ref=here, send_sem=fours_send.at[j], recv_sem=fours_recv.at[j],
            device_id={"traces": ((z + away) % chips) * 2 + core}, device_id_type=MESH,
        )

    def pass_copy():
        return pltpu.make_async_remote_copy(
            src_ref=bank.at[half, core, :, :, four], dst_ref=bank.at[half, core, :, :, four], send_sem=pass_sem.at[0], recv_sem=pass_sem.at[1],
            device_id={"traces": z * 2 + 1 - core}, device_id_type=MESH,
        )

    other = {"groups": group + 1 - 2 * half, "traces": me}
    far_other = {"groups": group + 2 - 4 * pair, "traces": me}

    def cross_copy():
        return pltpu.make_async_remote_copy(
            src_ref=bank.at[half, :, :, :, four], dst_ref=bank.at[half, :, :, :, four],
            send_sem=pass_sem.at[2], recv_sem=pass_sem.at[3], device_id=other, device_id_type=MESH,
        )

    def far_cross_copy():
        return pltpu.make_async_remote_copy(
            src_ref=bank.at[:, :, :, :, four], dst_ref=bank.at[:, :, :, :, four],
            send_sem=pass_sem.at[4], recv_sem=pass_sem.at[5], device_id=far_other, device_id_type=MESH,
        )

    right = lax.rem(z + 1, chips) * 2
    left = lax.rem(z + (chips - 1), chips) * 2
    barrier = pltpu.get_barrier_semaphore()
    for there in (right + core, left + core, right + 1 - core, left + 1 - core, z * 2 + 1 - core):
        pl.semaphore_signal(barrier, inc=1, device_id={"traces": there}, device_id_type=MESH)
    for there in (other, far_other):
        pl.semaphore_signal(barrier, inc=1, device_id=there, device_id_type=MESH)
    pl.semaphore_wait(barrier, 7)

    def tell(side):
        there = (right if side == 0 else left) + core
        pl.semaphore_signal(word.at[side], inc=1, device_id={"traces": there}, device_id_type=MESH)

    tell(0)
    tell(1)
    for k in (2, 3, 4, 5, 1):
        raw_copy(k).start()
    small = [
        pltpu.make_async_copy(index_hbm, index_ref, table_sem.at[2]),
        pltpu.make_async_copy(damp_hbm, damp_ref, table_sem.at[3]),
        pltpu.make_async_copy(own_taps, bank.at[half, core, z % 4, z // 4, four], table_sem.at[4]),
    ]
    for copy in small:
        copy.start()

    def hear(_, __):
        for side in (0, 1):
            pl.semaphore_wait(word.at[side], 1)
            tell(side)
        return 0

    lax.fori_loop(0, chips // 2 - 2, hear, 0)
    for side in (0, 1):
        pl.semaphore_wait(word.at[side], 1)

    def start_note(k, _):
        note_copy(k).start()
        return 0

    def start_raw(k, _):
        raw_copy(k).start()
        return 0

    def start_late(k, _):
        for i in range(8):
            late_copy(k, i * PITCH, 64).start()
        return 0

    def start_input(k, _):
        late_input(k).start()
        return 0

    def wait_note(k, _):
        note_copy(k).wait()
        return 0

    def wait_input(k, _):
        late_input(k).wait()
        return 0

    for j in range(1, chips // 4):
        wave_copy(j).start()
    for k in (8, 9):
        raw_copy(k).start()
    own_copy = pltpu.make_async_copy(x_ref.at[eight_rows(me)], raw.at[0], own_sem.at[LATE])
    own_copy.start()
    across_copy = pltpu.make_async_copy(across_ref, across, table_sem.at[0])
    across_copy.start()
    twist_copy = pltpu.make_async_copy(twist_ref, twist, table_sem.at[1])
    twist_copy.start()
    lax.fori_loop(n - LATE, n, start_input, 0)
    for copy in small:
        copy.wait()
    lane = lax.broadcasted_iota(jnp.int32, (1, 128), 1)
    damp = jnp.zeros((1, 128), jnp.float32)
    for i in range(8):
        damp = jnp.where(lane == 8 + i, damp_ref[i], damp)

    def fill(e, _):
        row = damp
        for i in range(8):
            row = jnp.where(lane == i, index_ref[e * 8 + i].astype(jnp.float32), row)
        own[e] = row
        return 0

    lax.fori_loop(0, n, fill, 0)
    note[mine] = own[me]
    for j in range(1, chips // 4):
        wave_copy(j).wait()
    for j in (1, 2, 3):
        fours_copy(j).start()
    lax.fori_loop(1, n, start_note, 0)
    lax.fori_loop(6, 8, start_raw, 0)
    lax.fori_loop(10, n - LATE, start_raw, 0)
    own_copy.wait()
    across_copy.wait()
    twist_copy.wait()
    lax.fori_loop(n - LATE, n, wait_input, 0)
    for j in (1, 2, 3):
        fours_copy(j).wait()
    pass_copy().start()
    lax.fori_loop(1, n, wait_note, 0)
    pass_copy().wait()
    cross_copy().start()
    cross_copy().wait()
    far_cross_copy().start()
    far_cross_copy().wait()

    lanes = lax.broadcasted_iota(jnp.int32, (n, 8, 128), 2)
    place = lax.broadcasted_iota(jnp.int32, (n, 8, 128), 1)

    def spread(notes, at):
        return jnp.sum(jnp.where(lanes == place + at, notes, 0.0), axis=2, keepdims=True).reshape(8 * n, 1)

    damping = spread(note[...], 8)
    every = jnp.concatenate([bank[0].reshape(8 * n, 128), bank[1].reshape(8 * n, 128)], axis=1)
    level = jnp.sum(every * every, axis=1, keepdims=True)
    water = jnp.broadcast_to(damping * (level + 1e-6), (8 * n, 128))
    slot = lax.broadcasted_iota(jnp.int32, (8 * n, 8 * n), 1)
    chip = ((slot // 8) % (chips // 4)) * 4 + (slot // (2 * chips)) % 4
    ids = chip * 16 + (slot // (8 * chips)) * 8 + slot % 8
    for half, notes in enumerate((note, own)):
        pick = jnp.where(spread(notes[...], 0) == ids.astype(jnp.float32), 1.0, 0.0).astype(jnp.float32)
        here = pl.ds(half * n, n)
        taps[here] = jnp.dot(pick, every, precision=HIGHEST, preferred_element_type=jnp.float32).reshape(n, 8, 256)
        floors[here] = jnp.dot(pick, water, precision=HIGHEST, preferred_element_type=jnp.float32).reshape(n, 8, 128)

    def block(i, _):
        k = (i + n - LATE) % n
        raws = (i + n - LATE) // n
        sz, sc = source(k)

        @pl.when(i > LATE)
        def _():
            raw_copy(k).wait_recv()

        @pl.when(i == LATE + 1)
        def _():
            lax.fori_loop(n - LATE, n, start_late, 0)

        out = raws * (sz * 2 + sc) + (1 - raws) * (n + i)
        p = raws * place_of(sz, sc) + (1 - raws) * (n + target(k))
        deconvolve(raw.at[k], o_ref.at[out], taps.at[p], floors.at[p], across, twist, part, lhs, spec)
        return 0

    lax.fori_loop(0, n, block, 0)

    def finish_raw(k, _):
        raw_copy(k).wait_send()
        return 0

    def finish_late(k, _):
        late_copy(k, 0, 512).wait()
        return 0

    lax.fori_loop(1, n - LATE, finish_raw, 0)
    lax.fori_loop(n - LATE, n, finish_late, 0)


def exchange(n, x, index, damp, wave, across, twist):
    rows, length = x.shape
    hbm = pl.BlockSpec(memory_space=pltpu.HBM)
    f32 = jnp.float32
    dma = pltpu.SemaphoreType.DMA
    return pl.pallas_call(
        functools.partial(exchange_kernel, n),
        out_shape=jax.ShapeDtypeStruct((n + LATE, 8 * PITCH, 128), f32),
        in_specs=[hbm] * 6,
        out_specs=pl.BlockSpec(memory_space=pltpu.VMEM),
        scratch_shapes=[
            pltpu.SMEM(index.shape, jnp.int32),
            pltpu.SMEM(damp.shape, f32),
            pltpu.VMEM((n, 8, length), f32),
            pltpu.VMEM((n, 1, 128), f32),
            pltpu.VMEM((n, 1, 128), f32),
            pltpu.VMEM((2, 2, 4, n // 8, 8, 128), f32),
            pltpu.VMEM((2 * n, 8, 256), f32),
            pltpu.VMEM((2 * n, 8, 128), f32),
            pltpu.VMEM(across.shape, f32),
            pltpu.VMEM(twist.shape, f32),
            pltpu.VMEM((8, 8, 8, 128), f32),
            pltpu.VMEM((2 * NK, 8, 256), f32),
            pltpu.VMEM((2 * NK, 8, 256), f32),
            dma((n,)), dma((n,)), dma((n,)), dma((n,)), dma((n // 8,)), dma((n // 8,)), dma((4,)), dma((4,)), dma((6,)),
            dma((LATE + 1,)), dma((5,)), pltpu.SemaphoreType.REGULAR((2,)),
        ],
        compiler_params=pltpu.CompilerParams(collective_id=0, has_side_effects=True, vmem_limit_bytes=VMEM_LIMIT),
    )(*(pltpu.with_memory_space_constraint(a, pltpu.HBM) for a in (x, index, damp, wave, across, twist)))


def reorder_kernel(n, order_ref, x_ref, o_ref, *scratch):
    *helds, lined, out_sem = scratch
    rows = o_ref.shape[0]
    tiles = rows // 8

    def out_copy(t):
        here = pl.ds(pl.multiple_of(t * 8, 8), 8)
        return pltpu.make_async_copy(lined.at[here], o_ref.at[here], out_sem)

    def line_up(g, _):
        for u, held in enumerate(helds):
            t = g * len(helds) + u
            for i in range(8):
                p = order_ref[t * 8 + i]
                held[pl.ds(i * PITCH, 64), :] = x_ref[p % n, pl.ds((p // n) * PITCH, 64), :]
        for u, held in enumerate(helds):
            t = g * len(helds) + u
            here = pl.ds(pl.multiple_of(t * 8, 8), 8)
            for i in range(64):
                lined[here, pl.ds(i * 128, 128)] = held[pl.ds(i, 8, stride=PITCH), :]
            out_copy(t).start()
        return 0

    lax.fori_loop(0, tiles // len(helds), line_up, 0)

    pltpu.make_async_copy(lined, o_ref, out_sem).wait()


def reorder(n, order, x):
    rows, length = order.shape[0], 8192
    return pl.pallas_call(
        functools.partial(reorder_kernel, n),
        out_shape=jax.ShapeDtypeStruct((rows, length), x.dtype),
        in_specs=[pl.BlockSpec(memory_space=pltpu.SMEM), pl.BlockSpec(memory_space=pltpu.VMEM)],
        out_specs=pl.BlockSpec(memory_space=pl.ANY),
        scratch_shapes=[
            *[pltpu.VMEM((8 * PITCH, 128), x.dtype)] * 4,
            pltpu.VMEM((rows, length), x.dtype),
            pltpu.SemaphoreType.DMA,
        ],
        compiler_params=pltpu.CompilerParams(vmem_limit_bytes=VMEM_LIMIT),
    )(order, x)


def solution(mesh):
    n = mesh.shape["traces"]
    across, twist = tables()

    def local(raw_traces, filter_index, channel_order, wavelets, damping):
        moved = exchange(n, raw_traces, filter_index, damping, wavelets, jnp.asarray(across), jnp.asarray(twist))
        return reorder(n, channel_order, moved)

    placed = (
        P(("groups", "traces"), None),
        P(("groups", "traces")),
        P("groups"),
        P("traces", None),
        P("traces"),
    )
    return jax.shard_map(
        local, mesh=mesh, in_specs=placed, out_specs=P(("groups", "traces"), None), check_vma=False
    )
```
